32 devices in a mesh: expert: 8 (over z, x), shard: 4 (over y, core).
Axes of the slice: x: 2, y: 2, z: 4, core: 2. Of those that a mesh axis runs over, the one named last changes fastest.
Arguments:
- tokens_in: bfloat16 [4096, 2048], P(('expert', 'shard')), may hold values from -6 to 6
- out_grad: bfloat16 [4096, 2048], P(('expert', 'shard')), may hold values from -6 to 6
- segment_ids: int32 [8, 512], P('expert'), may hold values from 0 to 3, never falling along the last dimension, each value on 1 to 256 neighbouring positions
- expert_ids: int32 [4096, 8], P(('expert', 'shard')), may hold values from 0 to 31, all different within a row; in each aligned block of 128 rows (0 to 127, 128 to 255, ...) at most 64 rows name the same one
- route_weights: float32 [4096, 8], P(('expert', 'shard')), may hold values from 0.2 to 0.6
- attn_gain: bfloat16 [2048], P(('expert', 'shard')), may hold values from 0.5 to 2
- qkv_weight: bfloat16 [2048, 5120], P(('expert', 'shard')), may hold values from -0.125 to 0.125
- q_gain: bfloat16 [128], P(('expert', 'shard')), may hold values from 0.5 to 2
- k_gain: bfloat16 [128], P(('expert', 'shard')), may hold values from 0.5 to 2
- out_weight: bfloat16 [4096, 2048], P(('expert', 'shard')), may hold values from -0.75 to 0.75
- moe_gain: bfloat16 [2048], P(('expert', 'shard')), may hold values from 0.5 to 2
- expert_in: bfloat16 [32, 2048, 1536], P(('expert', 'shard')), may hold values from -0.125 to 0.125
- expert_out: bfloat16 [32, 768, 2048], P(('expert', 'shard')), may hold values from -0.4375 to 0.4375
Outputs:
- block_output: bfloat16 [4096, 2048], P(('expert', 'shard'))
- input_grad: bfloat16 [4096, 2048], P(('expert', 'shard'))
- attn_gain_grad: float32 [2048], P(('expert', 'shard'))
- qkv_weight_grad: float32 [2048, 5120], P(('expert', 'shard'))
- q_gain_grad: float32 [128], P(('expert', 'shard'))
- k_gain_grad: float32 [128], P(('expert', 'shard'))
- out_weight_grad: float32 [4096, 2048], P(('expert', 'shard'))
- moe_gain_grad: float32 [2048], P(('expert', 'shard'))
- expert_in_grad: float32 [32, 2048, 1536], P(('expert', 'shard'))
- expert_out_grad: float32 [32, 768, 2048], P(('expert', 'shard'))
The draws below stay inside these ranges and needn't reach their ends.
Inputs may be any that keep to these rules, and one draw needn't show every extreme that they name: `segment_ids`: within each pack the document numbers never fall; each document covers 1 to 256 tokens and one covers exactly 256. `expert_ids`: each token names 8 different experts. Among the 128 tokens of one device no expert is named more than 64 times, a bound that some block reaches.
All inputs are finite; a program needn't handle non-finite values.
Results may differ from the reference program's by a relative error of at most 0.022.
Values may be sent and summed in bfloat16 or wider, within the bound.
A program may use at most 384 MiB of HBM per device.

```python
import math
import jax
import jax.numpy as jnp
import numpy as np
from jax import lax

D = 2048
QUERY_HEADS = 32
KEY_VALUE_HEADS = 4
HEAD_DIMENSION = 128
FFE = 768
TOP = 8
TOK_DEV = 128
DOCS = 4
EXPERTS = 32
CAP = 64
PACK = 512
SEG_MOST = 256
QKV = 5120
TOKENS = 4096
N_EXPERT = 8
DEVICES = 32


def level_of(stream_key, shape, split, least, top_value):
    loudness, own = 1.0, jax.random.fold_in(stream_key, 6)
    for dim, blocks in split:
        heights = jnp.exp(jax.random.uniform(jax.random.fold_in(own, dim), (blocks,), jnp.float32, least / len(split), top_value / len(split)))
        loudness = loudness * jnp.repeat(heights, shape[dim] // blocks).reshape([-1 if axis == dim else 1 for axis in range(len(shape))])
    return loudness


def length_profile(amount, total, limit, slope):
    weights = [(1 << 20) // math.isqrt(grade ** slope) + 1 for grade in range(2, amount + 1)]
    rest, given = total - limit - (amount - 1), [1] * (amount - 1)
    while rest > 0:
        movable = [i for i in range(amount - 1) if given[i] < limit]
        pool, left = sum([weights[i] for i in movable]), rest
        for i in movable:
            addition = min(limit - given[i], max(1, left * weights[i] // pool), rest)
            given[i] = given[i] + addition
            rest = rest - addition
    return np.array([limit] + given)


def uneven(stream_key, number_of, total, reach, skew):
    if number_of == 2:
        one = jax.random.randint(stream_key, (), max(1, total - reach), min(reach, total - 1) + 1)
        return jnp.stack([one, total - one])
    tallies = jnp.asarray(length_profile(number_of, total, reach, skew), jnp.int32)
    pairs = (number_of - 1) // 2
    giver, taker = tallies[1:1 + 2 * pairs:2], tallies[2:2 + 2 * pairs:2]
    room = jnp.minimum(giver - 1, reach - taker)
    moved = jax.random.randint(jax.random.fold_in(stream_key, 1), (pairs,), 0, 1 << 20) % (room + 1)
    tallies = tallies.at[1:1 + 2 * pairs:2].set(giver - moved).at[2:2 + 2 * pairs:2].set(taker + moved)
    return tallies[jax.random.permutation(jax.random.fold_in(stream_key, 2), number_of)]


def routed_block(key, own, number, rows, count, top, most, slope):
    sequence = jax.random.permutation(key, count)
    packed, usual = portions_of(count, rows * top, most, slope, True), portions_of(count, rows * top, most, slope, False)
    places = jnp.arange(count)

    def named(tallies, rotation):
        used = int((tallies > 0).sum())
        fixed = max(1, used // 4)
        moved = fixed + (places - fixed + rotation * (used - fixed)) % max(1, count - fixed)
        return jnp.zeros((count,), jnp.int32).at[sequence[jnp.where(places < fixed, places, moved)]].set(jnp.asarray(tallies, jnp.int32))

    tallies = jnp.where(number % 4 == 0, named(packed, number // 4), named(usual, number - number // 4 - 1))
    mixed = jax.random.permutation(jax.random.fold_in(own, 3), count)
    giver, taker = mixed[0:count // 2 * 2:2], mixed[1:count // 2 * 2:2]
    slack = jnp.minimum(tallies[giver] - 1, most - tallies[taker]) // 2
    slack = jnp.where((giver == sequence[0]) | (taker == sequence[0]) | (tallies[taker] == 0), 0, jnp.maximum(slack, 0))
    moved = jax.random.randint(jax.random.fold_in(own, 4), (count // 2,), 0, 1 << 20) % (slack + 1)
    tallies = tallies.at[giver].add(-moved).at[taker].add(moved)
    members = jnp.searchsorted(jnp.cumsum(tallies), jnp.arange(rows * top), side="right").astype(jnp.int32)
    listing = members.reshape(top, rows).T
    listing = listing[jax.random.permutation(jax.random.fold_in(own, 1), rows)]
    rotation = jax.random.randint(jax.random.fold_in(own, 2), (rows, 1), 0, top)
    return jnp.take_along_axis(listing, (jnp.arange(top)[None, :] + rotation) % top, axis=1)


def portions_of(count, total, most, skew, full):
    portions = [(1 << 20) // math.isqrt(standing ** skew) + 1 for standing in range(1, count + 1)]
    largest = most if full else min(most, max(-(-total // count), total * portions[0] // sum(portions)))
    least = 1 if total - largest >= count - 1 else 0
    counts, rest = [largest] + [least] * (count - 1), total - largest - least * (count - 1)
    while rest > 0:
        candidates = [i for i in range(1, count) if counts[i] < largest] or [i for i in range(1, count) if counts[i] < most]
        mass, budget = sum([portions[i] for i in candidates]), rest
        for i in candidates:
            extra = min(most - counts[i], max(1, budget * portions[i] // mass), rest)
            counts[i] = counts[i] + extra
            rest = rest - extra
    return np.array(counts)


def normal_values(own_key, extent, deviation, most, split=(), held_as=jnp.bfloat16):
    loudness = level_of(own_key, extent, split, -0.22, 0.18) if split else 1.0
    drawn = jax.random.normal(own_key, extent, jnp.float32) * deviation * loudness
    return jnp.minimum(jnp.maximum(drawn, -most), most).astype(held_as)


def setup_inputs(seed: int = 0) -> dict:
    arg_keys = jax.random.split(jax.random.key(seed), 14)
    tokens_in = normal_values(arg_keys[0], (TOKENS, D), 1.0, 6.0, ((0, 32),))
    out_grad = normal_values(arg_keys[1], (TOKENS, D), 1.0, 6.0, ((0, 32),))
    segment_ids = jax.vmap(lambda own: jnp.searchsorted(jnp.cumsum(uneven(own, DOCS, PACK, SEG_MOST, 2)), jnp.arange(PACK), side="right"))(jax.random.split(arg_keys[2], N_EXPERT)).reshape((N_EXPERT, PACK)).astype(jnp.int32)
    expert_ids_keys = jax.random.split(jax.random.fold_in(arg_keys[3], 1), TOKENS // TOK_DEV)
    expert_ids_turns = jax.random.permutation(jax.random.fold_in(arg_keys[3], 3), TOKENS // TOK_DEV)
    expert_ids = jax.vmap(lambda own, number: routed_block(jax.random.fold_in(arg_keys[3], 2), own, number, TOK_DEV, EXPERTS, TOP, CAP, 1))(expert_ids_keys, expert_ids_turns).reshape((TOKENS, TOP))
    route_weights = jnp.clip(0.2 + 0.400000021 * jax.random.uniform(arg_keys[4], (TOKENS, TOP), jnp.float32) ** level_of(arg_keys[4], (TOKENS, TOP), ((0, 32),), -0.2, 0.2), 0.2, 0.6)
    attn_gain = jnp.clip(jnp.exp(math.log(2.0) - 1.3862944 * jax.random.uniform(arg_keys[5], (D,), jnp.float32) ** level_of(arg_keys[5], (D,), ((0, 32),), -0.2, 0.2)), 0.5, 2.0).astype(jnp.bfloat16)
    qkv_weight = normal_values(arg_keys[6], (D, QKV), D ** -0.5, 0.125, ((0, 32),))
    q_gain = jnp.clip(jnp.exp(math.log(2.0) - 1.3862944 * jax.random.uniform(arg_keys[7], (HEAD_DIMENSION,), jnp.float32) ** level_of(arg_keys[7], (HEAD_DIMENSION,), ((0, 32),), -0.2, 0.2)), 0.5, 2.0).astype(jnp.bfloat16)
    k_gain = jnp.clip(jnp.exp(math.log(2.0) - 1.3862944 * jax.random.uniform(arg_keys[8], (HEAD_DIMENSION,), jnp.float32) ** level_of(arg_keys[8], (HEAD_DIMENSION,), ((0, 32),), -0.2, 0.2)), 0.5, 2.0).astype(jnp.bfloat16)
    out_weight = normal_values(arg_keys[9], (QUERY_HEADS * HEAD_DIMENSION, D), (QUERY_HEADS * HEAD_DIMENSION // 64) ** -0.5, 0.75, ((0, 32),))
    moe_gain = jnp.clip(jnp.exp(math.log(2.0) - 1.3862944 * jax.random.uniform(arg_keys[10], (D,), jnp.float32) ** level_of(arg_keys[10], (D,), ((0, 32),), -0.2, 0.2)), 0.5, 2.0).astype(jnp.bfloat16)
    expert_in = normal_values(arg_keys[11], (EXPERTS, D, 2 * FFE), D ** -0.5, 0.125, ((0, 32),))
    expert_out = normal_values(arg_keys[12], (EXPERTS, FFE, D), (FFE // 4) ** -0.5, 0.4375, ((0, 32),))
    return {"tokens_in": tokens_in, "out_grad": out_grad, "segment_ids": segment_ids, "expert_ids": expert_ids, "route_weights": route_weights, "attn_gain": attn_gain, "qkv_weight": qkv_weight, "q_gain": q_gain, "k_gain": k_gain, "out_weight": out_weight, "moe_gain": moe_gain, "expert_in": expert_in, "expert_out": expert_out}


EPSILON = 1e-06
THETA = 1000000.0

def norm_rows(values_in, gain):
    return values_in * lax.rsqrt(lax.optimization_barrier(jnp.mean(values_in * values_in, axis=-1, keepdims=True)) + EPSILON) * gain

def rotate(vectors, position):
    half_size = vectors.shape[-1] // 2
    freqs = jnp.exp(jnp.arange(half_size, dtype=jnp.float32) * (-2.0 * math.log(THETA) / vectors.shape[-1]))
    angles = position[:, None] * freqs[None, :]
    cosine = jnp.cos(angles)[:, None, :]
    sine = jnp.sin(angles)[:, None, :]
    first = vectors[..., :half_size]
    second = vectors[..., half_size:]
    return jnp.concatenate([first * cosine - second * sine, second * cosine + first * sine], axis=-1)

def prepare(query_raw, unrotated_key, query_gain, key_gain, position):
    return (rotate(norm_rows(query_raw, query_gain), position), rotate(norm_rows(unrotated_key, key_gain), position))

def segment_positions(segment):
    index = jnp.arange(segment.shape[0], dtype=jnp.int32)
    change = jnp.concatenate([jnp.ones((1,), dtype=bool), segment[1:] != segment[:-1]])
    start = lax.cummax(jnp.where(change, index, 0), axis=0)
    return index - start

def scores_of(queries, key_row_block, allowed):
    tok_count, heads, head_size = queries.shape
    kv_heads = key_row_block.shape[1]
    grouped = queries.reshape(tok_count, kv_heads, heads // kv_heads, head_size).astype(jnp.float32)
    scores = jnp.einsum('tkgd,skd->kgts', grouped, key_row_block.astype(jnp.float32)) * head_size ** (-0.5)
    return (jnp.where(allowed[None, None], scores, -1e+30), grouped)

def attend(queries, key_row_block, value_row_block, allowed):
    scores, grouped = scores_of(queries, key_row_block, allowed)
    highest = lax.optimization_barrier(jnp.max(scores, axis=-1, keepdims=True))
    log_total = highest + jnp.log(lax.optimization_barrier(jnp.sum(jnp.exp(scores - highest), axis=-1, keepdims=True)))
    probs = jnp.exp(scores - log_total).astype(jnp.bfloat16)
    mixed = jnp.einsum('kgts,skd->tkgd', probs.astype(jnp.float32), value_row_block.astype(jnp.float32))
    return (mixed.reshape(queries.shape[0], -1).astype(jnp.bfloat16), log_total)

def attend_back(queries, key_row_block, value_row_block, allowed, log_total, attn_out, attn_grad):
    tok_count, heads, head_size = queries.shape
    kv_heads = key_row_block.shape[1]
    scores, grouped = scores_of(queries, key_row_block, allowed)
    probs = jnp.exp(scores - log_total)
    probs_low = probs.astype(jnp.bfloat16)
    grad_heads = attn_grad.reshape(tok_count, kv_heads, heads // kv_heads, head_size).astype(jnp.float32)
    out_heads = attn_out.reshape(tok_count, kv_heads, heads // kv_heads, head_size).astype(jnp.float32)
    delta = jnp.einsum('tkgd,tkgd->kgt', grad_heads, out_heads)
    prob_grad = jnp.einsum('tkgd,skd->kgts', grad_heads, value_row_block.astype(jnp.float32))
    score_grad = (probs * (prob_grad - delta[..., None])).astype(jnp.bfloat16).astype(jnp.float32)
    factor = head_size ** (-0.5)
    query_grad = jnp.einsum('kgts,skd->tkgd', score_grad, key_row_block.astype(jnp.float32)).reshape(tok_count, heads, head_size) * factor
    key_gradient = jnp.einsum('kgts,tkgd->skd', score_grad, grouped) * factor
    value_grad = jnp.einsum('kgts,tkgd->skd', probs_low.astype(jnp.float32), grad_heads)
    return (query_grad, key_gradient, value_grad)

def expert_step(rows_in, row_grads, weight_in, weight_out):
    hidden_size = weight_out.shape[0]
    pre = jnp.dot(rows_in, weight_in, preferred_element_type=jnp.float32)
    gate_part = pre[:, :hidden_size]
    up_part = pre[:, hidden_size:]
    sigma = jax.nn.sigmoid(gate_part)
    active = gate_part * sigma
    hidden = (active * up_part).astype(jnp.bfloat16)
    outputs = jnp.dot(hidden, weight_out, preferred_element_type=jnp.float32).astype(jnp.bfloat16)
    hidden_grad = jnp.dot(row_grads, weight_out.T, preferred_element_type=jnp.float32)
    gate_grad = hidden_grad * up_part * (sigma * (1.0 + gate_part * (1.0 - sigma)))
    up_grad = hidden_grad * active
    pre_grad = jnp.concatenate([gate_grad, up_grad], axis=-1).astype(jnp.bfloat16)
    rows_grad = jnp.dot(pre_grad, weight_in.T, preferred_element_type=jnp.float32).astype(jnp.bfloat16)
    return (outputs, rows_grad, pre_grad, hidden)

def attention_forward(block_in, segment, attn_scale, qkv_weight, query_gain, key_gain, out_weight):
    packed_length = block_in.shape[0]
    block_f32 = block_in.astype(jnp.float32)
    normed_in = norm_rows(block_f32, attn_scale).astype(jnp.bfloat16)
    projected_rows = jnp.dot(normed_in, qkv_weight, preferred_element_type=jnp.float32)
    query_raw = projected_rows[:, :QUERY_HEADS * HEAD_DIMENSION].reshape(packed_length, QUERY_HEADS, HEAD_DIMENSION)
    unrotated_key = projected_rows[:, QUERY_HEADS * HEAD_DIMENSION:(QUERY_HEADS + KEY_VALUE_HEADS) * HEAD_DIMENSION].reshape(packed_length, KEY_VALUE_HEADS, HEAD_DIMENSION)
    value_row_block = projected_rows[:, (QUERY_HEADS + KEY_VALUE_HEADS) * HEAD_DIMENSION:].reshape(packed_length, KEY_VALUE_HEADS, HEAD_DIMENSION).astype(jnp.bfloat16)
    position = segment_positions(segment).astype(jnp.float32)
    query_rot, key_rot = prepare(query_raw, unrotated_key, query_gain, key_gain, position)
    index = jnp.arange(packed_length, dtype=jnp.int32)
    allowed = (segment[:, None] == segment[None, :]) & (index[None, :] <= index[:, None])
    query_low = query_rot.astype(jnp.bfloat16)
    key_low = key_rot.astype(jnp.bfloat16)
    attn_out, log_total = attend(query_low, key_low, value_row_block, allowed)
    hidden_state = block_f32 + jnp.dot(attn_out, out_weight, preferred_element_type=jnp.float32)
    return (block_f32, normed_in, query_raw, unrotated_key, value_row_block, position, query_low, key_low, allowed, attn_out, log_total, hidden_state)

def reference(tokens_in, out_grad, segment_ids, expert_ids, route_weights, attn_gain, qkv_weight, q_gain, k_gain, out_weight, moe_gain, expert_in, expert_out):
    attn_scale = attn_gain.astype(jnp.float32)
    query_gain = q_gain.astype(jnp.float32)
    key_gain = k_gain.astype(jnp.float32)
    moe_scale = moe_gain.astype(jnp.float32)
    packs_in = tokens_in.reshape(N_EXPERT, PACK, D)

    def forward_pack(inputs):
        block_in, segment = inputs
        kept = attention_forward(block_in, segment, attn_scale, qkv_weight, query_gain, key_gain, out_weight)
        hidden_state = kept[11]
        return (hidden_state, norm_rows(hidden_state, moe_scale).astype(jnp.bfloat16))
    hidden_all, moe_in_all = lax.map(forward_pack, (packs_in, segment_ids))
    hidden_all = hidden_all.reshape(TOKENS, D)
    moe_in_all = moe_in_all.reshape(TOKENS, D)
    flat_ids = expert_ids.reshape(DEVICES, TOK_DEV * TOP)

    def ranks_of(ids_here):
        one_hot = (ids_here[:, None] == jnp.arange(EXPERTS, dtype=jnp.int32)[None, :]).astype(jnp.int32)
        return lax.optimization_barrier(jnp.sum((jnp.cumsum(one_hot, axis=0) - 1) * one_hot, axis=1))
    ranks = jax.vmap(ranks_of)(flat_ids)
    device_index = jnp.arange(DEVICES, dtype=jnp.int32)[:, None]
    slot_global = flat_ids * (DEVICES * CAP) + device_index * CAP + ranks
    route_total = TOKENS * TOP
    table = jnp.full((EXPERTS * DEVICES * CAP,), route_total, dtype=jnp.int32)
    table = table.at[slot_global.reshape(-1)].set(jnp.arange(route_total, dtype=jnp.int32))
    table = table.reshape(EXPERTS, DEVICES * CAP)
    moe_pad = jnp.concatenate([moe_in_all, jnp.zeros((1, D), jnp.bfloat16)], axis=0)
    grad_pad = jnp.concatenate([out_grad.astype(jnp.float32), jnp.zeros((1, D), jnp.float32)], axis=0)
    weight_pad = jnp.concatenate([route_weights.reshape(-1), jnp.zeros((1,), jnp.float32)], axis=0)

    def expert_pass(carry, inputs):
        out_sum, in_sum = carry
        route_index, weight_in, weight_out = inputs
        token_index = jnp.where(route_index < route_total, route_index // TOP, TOKENS).astype(jnp.int32)
        gate_weight = weight_pad[route_index]
        rows_in = moe_pad[token_index]
        row_grads = (gate_weight[:, None] * grad_pad[token_index]).astype(jnp.bfloat16)
        outputs, rows_grad, pre_grad, hidden = expert_step(rows_in, row_grads, weight_in, weight_out)
        out_sum = out_sum.at[token_index].add(gate_weight[:, None] * outputs.astype(jnp.float32))
        in_sum = in_sum.at[token_index].add(rows_grad.astype(jnp.float32))
        in_weight_grad = jnp.dot(rows_in.T, pre_grad, preferred_element_type=jnp.float32)
        out_weight_grad = jnp.dot(hidden.T, row_grads, preferred_element_type=jnp.float32)
        return ((out_sum, in_sum), (in_weight_grad, out_weight_grad))
    start = (jnp.zeros((TOKENS + 1, D), jnp.float32), jnp.zeros((TOKENS + 1, D), jnp.float32))
    (out_sum, in_sum), (expert_in_grad, expert_out_grad) = lax.scan(expert_pass, start, (table, expert_in, expert_out))
    block_output = (hidden_all + out_sum[:TOKENS]).astype(jnp.bfloat16)

    def backward_pack(carry, inputs):
        block_in, segment, moe_grad, block_grad = inputs
        kept = attention_forward(block_in, segment, attn_scale, qkv_weight, query_gain, key_gain, out_weight)
        block_f32, normed_in, query_raw, unrotated_key, value_row_block, position, query_low, key_low, allowed, attn_out, log_total, hidden_state = kept
        norm_out, norm_back = jax.vjp(norm_rows, hidden_state, moe_scale)
        hidden_grad, moe_scale_grad = norm_back(moe_grad)
        residual_grad = block_grad.astype(jnp.float32) + hidden_grad
        residual_low = residual_grad.astype(jnp.bfloat16)
        out_term = jnp.dot(attn_out.T, residual_low, preferred_element_type=jnp.float32)
        attn_grad = jnp.dot(residual_low, out_weight.T, preferred_element_type=jnp.float32).astype(jnp.bfloat16)
        query_grad, key_gradient, value_grad = attend_back(query_low, key_low, value_row_block, allowed, log_total, attn_out, attn_grad)

        def prepare_here(query_in, key_in, gain_q, gain_k):
            return prepare(query_in, key_in, gain_q, gain_k, position)
        prep_out, prep_back = jax.vjp(prepare_here, query_raw, unrotated_key, query_gain, key_gain)
        query_raw_grad, key_raw_grad, query_gain_grad, key_gain_grad = prep_back((query_grad, key_gradient))
        packed_length = block_in.shape[0]
        projected_grad = jnp.concatenate([query_raw_grad.reshape(packed_length, -1), key_raw_grad.reshape(packed_length, -1), value_grad.reshape(packed_length, -1)], axis=1).astype(jnp.bfloat16)
        qkv_term = jnp.dot(normed_in.T, projected_grad, preferred_element_type=jnp.float32)
        normed_grad = jnp.dot(projected_grad, qkv_weight.T, preferred_element_type=jnp.float32)
        first_out, first_back = jax.vjp(norm_rows, block_f32, attn_scale)
        input_part, attn_scale_grad = first_back(normed_grad)
        pack_grad = (residual_grad + input_part).astype(jnp.bfloat16)
        sums = (carry[0] + attn_scale_grad, carry[1] + qkv_term, carry[2] + query_gain_grad, carry[3] + key_gain_grad, carry[4] + out_term, carry[5] + moe_scale_grad)
        return (sums, pack_grad)
    zeros_start = (jnp.zeros((D,), jnp.float32), jnp.zeros((D, QKV), jnp.float32), jnp.zeros((HEAD_DIMENSION,), jnp.float32), jnp.zeros((HEAD_DIMENSION,), jnp.float32), jnp.zeros((QUERY_HEADS * HEAD_DIMENSION, D), jnp.float32), jnp.zeros((D,), jnp.float32))
    grads, input_grad = lax.scan(backward_pack, zeros_start, (packs_in, segment_ids, in_sum[:TOKENS].reshape(N_EXPERT, PACK, D), out_grad.reshape(N_EXPERT, PACK, D)))
    input_grad = input_grad.reshape(TOKENS, D)
    return (block_output, input_grad, grads[0], grads[1], grads[2], grads[3], grads[4], grads[5], expert_in_grad, expert_out_grad)
```

```python
import math
import jax, jax.numpy as jnp
from jax import lax
from jax.experimental import pallas as pl
from jax.experimental.pallas import tpu as pltpu
from jax.sharding import PartitionSpec as P
MESH = pl.DeviceIdType.MESH
ANY = pl.BlockSpec(memory_space=pl.ANY)
VM = pl.BlockSpec(memory_space=pltpu.VMEM)

def grid_of():
    n_expert, n_shard = lax.axis_size("expert"), lax.axis_size("shard")
    ny = n_shard // 2
    nx = min(ny, n_expert)
    return n_expert // nx, nx, ny

class Place:
    def __init__(self):
        self.nz, self.nx, self.ny = grid_of()
        e, s = lax.axis_index("expert"), lax.axis_index("shard")
        self.z, self.x = e // self.nx, e % self.nx
        self.y, self.c = s // 2, s % 2
    def dev(self, dz=0, dx=0, dy=0, dc=0):
        z, x, y, c = self.at(dz, dx, dy, dc)
        return (z * self.nx + x, y * 2 + c)
    def at(self, dz=0, dx=0, dy=0, dc=0):
        z = lax.rem(self.z + dz + self.nz, self.nz) if dz else self.z
        x = lax.rem(self.x + dx + self.nx, self.nx) if dx else self.x
        y = lax.rem(self.y + dy + self.ny, self.ny) if dy else self.y
        c = 1 - self.c if dc else self.c
        return z, x, y, c
    def index(self, dz=0, dx=0, dy=0, dc=0):
        z, x, y, c = self.at(dz, dx, dy, dc)
        return ((z * self.nx + x) * self.ny + y) * 2 + c
    def greet(self, peers):
        barrier = pltpu.get_barrier_semaphore()
        for p in peers:
            pl.semaphore_signal(barrier, inc=1, device_id=self.dev(*p), device_id_type=MESH)
        pl.semaphore_wait(barrier, len(peers))
    def line_peers(self):
        return ([(d, 0, 0, 0) for d in range(1, self.nz)] + [(0, d, 0, 0) for d in range(1, self.nx)]
                + [(0, 0, d, 0) for d in range(1, self.ny)] + [(0, 0, 0, 1)])

class Pool:
    def __init__(self, sems):
        self.sems, self.used = sems, 0
    def take(self):
        self.used += 1
        return self.sems.at[self.used - 1]

def gather_all_kernel(b_ref, o_ref, local_sem, send, recv):
    p = Place()
    nz, nx, ny = p.nz, p.nx, p.ny
    half = b_ref.shape[0] // 2
    A, B = pl.ds(0, half), pl.ds(half, half)
    F = pl.ds(0, 2 * half)
    p.greet(p.line_peers())
    own = pltpu.make_async_copy(b_ref, o_ref.at[p.index()], local_sem)
    own.start()
    s, r = Pool(send), Pool(recv)
    sent = []
    def push(src_at, rows, to, first=False):
        i = p.index(*src_at)
        src = b_ref.at[rows] if first else o_ref.at[i, rows]
        cp = pltpu.make_async_remote_copy(src_ref=src, dst_ref=o_ref.at[i, rows], send_sem=s.take(),
            recv_sem=r.take(), device_id=p.dev(*to), device_id_type=MESH)
        cp.start()
        sent.append(cp)
        return cp
    neg = lambda d, n: (n - d) % n
    first = {}
    for d in range(1, nz):
        first[d] = push((0, 0, 0, 0), F, (d, 0, 0, 0), True)
    second_a, second_b, third, fourth = {}, {}, {}, []
    def stage_one(k):
        if k:
            first[k].wait_recv()
        at = (neg(k, nz), 0, 0, 0)
        for d in range(1, nx):
            second_a[k, d] = push(at, A, (0, d, 0, 0), k == 0)
        for d in range(1, ny):
            second_b[k, d] = push(at, B, (0, 0, d, 0), k == 0)
        for d in range(1, ny):
            third["a", k, 0, d] = push(at, A, (0, 0, d, 0), k == 0)
        for d in range(1, nx):
            third["b", k, 0, d] = push(at, B, (0, d, 0, 0), k == 0)
        fourth.append(push(at, F, (0, 0, 0, 1), k == 0))
    def stage_two(k):
        for dx in range(1, nx):
            second_a[k, dx].wait_recv()
            at = (neg(k, nz), neg(dx, nx), 0, 0)
            for d in range(1, ny):
                third["a", k, dx, d] = push(at, A, (0, 0, d, 0))
            fourth.append(push(at, A, (0, 0, 0, 1)))
        for dy in range(1, ny):
            second_b[k, dy].wait_recv()
            at = (neg(k, nz), 0, neg(dy, ny), 0)
            for d in range(1, nx):
                third["b", k, dy, d] = push(at, B, (0, d, 0, 0))
            fourth.append(push(at, B, (0, 0, 0, 1)))
    def stage_three(k):
        for dx in range(nx):
            for d in range(1, ny):
                third["a", k, dx, d].wait_recv()
                fourth.append(push((neg(k, nz), neg(dx, nx), neg(d, ny), 0), A, (0, 0, 0, 1)))
        for dy in range(ny):
            for d in range(1, nx):
                third["b", k, dy, d].wait_recv()
                fourth.append(push((neg(k, nz), neg(d, nx), neg(dy, ny), 0), B, (0, 0, 0, 1)))
    for k in range(nz + 2):
        if k < nz:
            stage_one(k)
        if 0 <= k - 1 < nz:
            stage_two(k - 1)
        if 0 <= k - 2 < nz:
            stage_three(k - 2)
    for cp in fourth:
        cp.wait_recv()
    for cp in sent:
        cp.wait_send()
    own.wait()

def gather_all(block, cid):
    nz, nx, ny = grid_of()
    return pl.pallas_call(gather_all_kernel,
        out_shape=jax.ShapeDtypeStruct((nz * nx * ny * 2,) + block.shape, block.dtype),
        in_specs=[VM], out_specs=ANY,
        scratch_shapes=[pltpu.SemaphoreType.DMA, pltpu.SemaphoreType.DMA((n_sems(nz, nx, ny),)), pltpu.SemaphoreType.DMA((n_sems(nz, nx, ny),))],
        compiler_params=pltpu.CompilerParams(collective_id=cid, has_side_effects=True),
        name="gather_all")(block)

def n_sems(nz, nx, ny):
    return (nz - 1) + nz * (nx - 1 + ny - 1 + 1) + nz * (nx * (ny - 1) + ny * (nx - 1)) + nz * (nx - 1 + ny - 1) + nz * (nx * (ny - 1) + ny * (nx - 1))

def reduce_all_kernel(g_ref, out_ref, acc, rc, ra1, rb1, ra2, rb2, rz, load_sem, send, recv):
    p = Place()
    nz, nx, ny = p.nz, p.nx, p.ny
    rows = g_ref.shape[1]
    half = rows // 2
    A, B = pl.ds(0, half), pl.ds(half, half)
    p.greet(p.line_peers())
    s, r = Pool(send), Pool(recv)
    sent = []
    order = [(dz, dx, dy) for dx in reversed(range(nx)) for dy in reversed(range(ny)) for dz in range(nz)]
    slot = lambda dz, dx, dy: (dz * nx + dx) * ny + dy
    neg = lambda d, n: (n - d) % n
    def push(src, dst, to):
        cp = pltpu.make_async_remote_copy(src_ref=src, dst_ref=dst, send_sem=s.take(), recv_sem=r.take(),
            device_id=p.dev(*to), device_id_type=MESH)
        cp.start()
        sent.append(cp)
        return cp
    loads, cores = {}, {}
    zs = list(range(1, nz)) + [0]
    plane = [(dx, dy) for dx in reversed(range(nx)) for dy in reversed(range(ny))]
    for dz in zs:
        for dx, dy in plane:
            k = (dz, dx, dy)
            i = slot(*k)
            cores[k] = push(g_ref.at[p.index(*k, 1)], rc.at[i], (0, 0, 0, 1))
            loads[k] = pltpu.make_async_copy(g_ref.at[p.index(*k)], acc.at[i], load_sem.at[i])
            loads[k].start()
    def add(dst, rows_, src):
        dst_v = acc[dst, rows_, :].astype(jnp.float32) + src[...].astype(jnp.float32)
        acc[dst, rows_, :] = dst_v.astype(acc.dtype)
    ca, cb, za, zb, zz = {}, {}, {}, {}, {}
    def stage_one(dz):
        for dx, dy in plane:
            k = (dz, dx, dy)
            i = slot(*k)
            loads[k].wait()
            cores[k].wait_recv()
            acc[i] = (acc[i].astype(jnp.float32) + rc[i].astype(jnp.float32)).astype(acc.dtype)
            if dy:
                ca[k] = push(acc.at[i, A], ra1.at[dy - 1, dz * nx + dx], (0, 0, dy, 0))
            if dx:
                cb[k] = push(acc.at[i, B], rb1.at[dx - 1, dz * ny + dy], (0, dx, 0, 0))
    def stage_two(dz):
        for dx in reversed(range(nx)):
            for dy in range(1, ny):
                ca[dz, dx, dy].wait_recv()
                add(slot(dz, dx, 0), A, ra1.at[dy - 1, dz * nx + dx])
            if dx:
                za[dz, dx] = push(acc.at[slot(dz, dx, 0), A], ra2.at[dx - 1, dz], (0, dx, 0, 0))
        for dy in reversed(range(ny)):
            for dx in range(1, nx):
                cb[dz, dx, dy].wait_recv()
                add(slot(dz, 0, dy), B, rb1.at[dx - 1, dz * ny + dy])
            if dy:
                zb[dz, dy] = push(acc.at[slot(dz, 0, dy), B], rb2.at[dy - 1, dz], (0, 0, dy, 0))
    def stage_three(dz):
        for dx in range(1, nx):
            za[dz, dx].wait_recv()
            add(slot(dz, 0, 0), A, ra2.at[dx - 1, dz])
        for dy in range(1, ny):
            zb[dz, dy].wait_recv()
            add(slot(dz, 0, 0), B, rb2.at[dy - 1, dz])
        if dz:
            zz[dz] = push(acc.at[slot(dz, 0, 0)], rz.at[dz - 1], (dz, 0, 0, 0))
    for k in range(nz + 2):
        if k < nz:
            stage_one(zs[k])
        if 0 <= k - 1 < nz:
            stage_two(zs[k - 1])
        if 0 <= k - 2 < nz:
            stage_three(zs[k - 2])
    total = acc[slot(0, 0, 0)].astype(jnp.float32)
    for dz in range(1, nz):
        zz[dz].wait_recv()
        total = total + rz[dz - 1].astype(jnp.float32)
    out_ref[...] = total.astype(out_ref.dtype)
    for cp in sent:
        cp.wait_send()

def reduce_all(terms, dtype, cid):
    nz, nx, ny = grid_of()
    nd, rows, width = terms.shape
    dt = terms.dtype
    half = rows // 2
    n = nz * nx * ny + 2 * nz * nx * ny + nz * (nx + ny) + nz
    blocks = 2 * nz * nx * ny + nz + (nz * (nx + 1) * (ny - 1) + nz * (ny + 1) * (nx - 1)) // 2 + 4
    parts = 1
    while blocks * rows * width * 2 // parts > 54 << 20:
        parts *= 2
    cols = width // parts
    one = pl.pallas_call(reduce_all_kernel,
        out_shape=jax.ShapeDtypeStruct((rows, cols), dtype),
        in_specs=[ANY], out_specs=VM,
        scratch_shapes=[pltpu.VMEM((nz * nx * ny, rows, cols), dt), pltpu.VMEM((nz * nx * ny, rows, cols), dt),
            pltpu.VMEM((ny - 1, nz * nx, half, cols), dt), pltpu.VMEM((nx - 1, nz * ny, half, cols), dt),
            pltpu.VMEM((nx - 1, nz, half, cols), dt), pltpu.VMEM((ny - 1, nz, half, cols), dt),
            pltpu.VMEM((nz - 1, rows, cols), dt),
            pltpu.SemaphoreType.DMA((nz * nx * ny,)), pltpu.SemaphoreType.DMA((n,)), pltpu.SemaphoreType.DMA((n,))],
        compiler_params=pltpu.CompilerParams(collective_id=cid, has_side_effects=True, vmem_limit_bytes=60 << 20),
        name="reduce_all")
    if parts == 1:
        return one(terms)
    return jnp.concatenate([one(terms[:, :, k * cols:(k + 1) * cols]) for k in range(parts)], axis=1)


def shard_peers(ny):
    return [(0, 0, dy, dc) for dy in range(ny) for dc in range(2) if dy or dc]


def weights_kernel(w_ref, wo_ref, t_ref, wall_ref, woall_ref, tall_ref, local_sem, send, recv):
    p = Place()
    nz, nx, ny = p.nz, p.nx, p.ny
    ns = ny * 2
    e, sh = lax.axis_index("expert"), lax.axis_index("shard")
    ne = nz * nx
    me = e * ns + sh
    to_e, to_s = me % ne, me // ne
    from_e, from_s = (sh * ne + e) // ns, (sh * ne + e) % ns
    moved = jnp.logical_not(jnp.logical_and(to_e == e, to_s == sh))
    peers = [q for q in p.line_peers() if not (q[2] or q[3])] + shard_peers(ny)
    barrier = pltpu.get_barrier_semaphore()
    for q in peers:
        pl.semaphore_signal(barrier, inc=1, device_id=p.dev(*q), device_id_type=MESH)

    @pl.when(moved)
    def _():
        pl.semaphore_signal(barrier, inc=1, device_id=(from_e, from_s), device_id_type=MESH)

    pl.semaphore_wait(barrier, len(peers) + moved.astype(jnp.int32))
    s, r = Pool(send), Pool(recv)
    sent = []
    neg = lambda d, n: (n - d) % n

    def push(src, dst, to):
        cp = pltpu.make_async_remote_copy(src_ref=src, dst_ref=dst, send_sem=s.take(), recv_sem=r.take(),
            device_id=p.dev(*to), device_id_type=MESH)
        cp.start()
        sent.append(cp)
        return cp

    mixed = []
    for q in shard_peers(ny):
        _, _, y, c = p.at(*q)
        mixed.append(push(w_ref.at[y * 2 + c], wall_ref.at[me], q))
    own_w = pltpu.make_async_copy(w_ref.at[sh], wall_ref.at[me], local_sem.at[0])
    own_w.start()
    entry_send, entry_recv = s.take(), r.take()
    entry = pltpu.make_async_remote_copy(src_ref=wo_ref, dst_ref=woall_ref.at[to_e], send_sem=entry_send,
        recv_sem=entry_recv, device_id=(to_e, to_s), device_id_type=MESH)
    stay = pltpu.make_async_copy(wo_ref, woall_ref.at[e], local_sem.at[1])

    @pl.when(moved)
    def _():
        entry.start()

    @pl.when(jnp.logical_not(moved))
    def _():
        stay.start()

    own_t = pltpu.make_async_copy(t_ref, tall_ref.at[sh], local_sem.at[2])
    own_t.start()
    toks = {}
    for d in range(1, ny):
        toks[d] = push(t_ref, tall_ref.at[sh], (0, 0, d, 0))
    tail = [push(t_ref, tall_ref.at[sh], (0, 0, 0, 1))]

    def block(ref, zz, size):
        z, x, _, _ = p.at(zz, 0, 0, 0)
        return ref.at[pl.ds((z * nx + x) * size, size)]

    def spread_first(ref, size):
        lines = {}
        for d in range(1, nz):
            b = block(ref, 0, size)
            lines[d] = push(b, b, (d, 0, 0, 0))
        for d in range(1, nx):
            b = block(ref, 0, size)
            tail.append(push(b, b, (0, d, 0, 0)))
        return lines

    def spread_next(ref, size, lines, d):
        lines[d].wait_recv()
        for dx in range(1, nx):
            b = block(ref, neg(d, nz), size)
            tail.append(push(b, b, (0, dx, 0, 0)))

    own_w.wait()
    for cp in mixed:
        cp.wait_recv()
    lines_w = spread_first(wall_ref, ns)

    @pl.when(moved)
    def _():
        entry.wait()

    @pl.when(jnp.logical_not(moved))
    def _():
        stay.wait()

    lines_o = spread_first(woall_ref, 1)
    for d in range(1, ny):
        toks[d].wait_recv()
        _, _, y, c = p.at(0, 0, neg(d, ny), 0)
        b = tall_ref.at[y * 2 + c]
        tail.append(push(b, b, (0, 0, 0, 1)))
    for d in range(1, nz):
        spread_next(wall_ref, ns, lines_w, d)
    for d in range(1, nz):
        spread_next(woall_ref, 1, lines_o, d)
    for cp in tail:
        cp.wait_recv()
    for cp in sent:
        cp.wait_send()
    own_t.wait()


def gather_weights(w, wo, t, cid):
    nz, nx, ny = grid_of()
    ns, ne = ny * 2, nz * nx
    n = 2 * ns + 2 + 2 * (nz + nx + nz * nx) + 2 * ny + 8
    return pl.pallas_call(weights_kernel,
        out_shape=(jax.ShapeDtypeStruct((ne * ns,) + w.shape[1:], w.dtype),
            jax.ShapeDtypeStruct((ne,) + wo.shape, wo.dtype), jax.ShapeDtypeStruct((ns,) + t.shape, t.dtype)),
        in_specs=[VM, VM, VM], out_specs=(ANY, ANY, ANY),
        scratch_shapes=[pltpu.SemaphoreType.DMA((3,)), pltpu.SemaphoreType.DMA((n,)), pltpu.SemaphoreType.DMA((n,))],
        compiler_params=pltpu.CompilerParams(collective_id=cid, has_side_effects=True),
        name="gather_weights")(w, wo, t)


def pack_gather_kernel(t_ref, o_ref, local_sem, send, recv):
    p = Place()
    ny = p.ny
    p.greet([(0, 0, d, 0) for d in range(1, ny)] + [(0, 0, 0, 1)])
    sh = lax.axis_index("shard")
    own = pltpu.make_async_copy(t_ref, o_ref.at[sh], local_sem)
    own.start()
    s, r = Pool(send), Pool(recv)
    sent, tail, along = [], [], {}
    rows = t_ref.shape[0]
    pieces = 4

    def push(src, dst, to):
        cp = pltpu.make_async_remote_copy(src_ref=src, dst_ref=dst, send_sem=s.take(), recv_sem=r.take(),
            device_id=p.dev(*to), device_id_type=MESH)
        cp.start()
        sent.append(cp)
        return cp

    part = [pl.ds(k * (rows // pieces), rows // pieces) for k in range(pieces)]
    for k in range(pieces):
        for d in range(1, ny):
            along[k, d] = push(t_ref.at[part[k]], o_ref.at[sh, part[k]], (0, 0, d, 0))
    tail.append(push(t_ref, o_ref.at[sh], (0, 0, 0, 1)))
    for k in range(pieces):
        for d in range(1, ny):
            along[k, d].wait_recv()
            _, _, y, c = p.at(0, 0, (ny - d) % ny, 0)
            b = o_ref.at[y * 2 + c, part[k]]
            tail.append(push(b, b, (0, 0, 0, 1)))
    for cp in tail:
        cp.wait_recv()
    for cp in sent:
        cp.wait_send()
    own.wait()


def pack_gather(t, cid):
    nz, nx, ny = grid_of()
    n = 8 * ny
    return pl.pallas_call(pack_gather_kernel,
        out_shape=jax.ShapeDtypeStruct((ny * 2,) + t.shape, t.dtype), in_specs=[VM], out_specs=VM,
        scratch_shapes=[pltpu.SemaphoreType.DMA, pltpu.SemaphoreType.DMA((n,)), pltpu.SemaphoreType.DMA((n,))],
        compiler_params=pltpu.CompilerParams(collective_id=cid, has_side_effects=True),
        name="pack_gather")(t)


def pack_reduce_body(p, g_ref, out_ref, acc, rc, ry, push, pieces=4):
    ny = p.ny
    rows = g_ref.shape[1]
    step = rows // pieces
    part = [pl.ds(k * step, step) for k in range(pieces)]
    order = list(range(1, ny)) + [0]
    cores, along = {}, {}
    for k in range(pieces):
        for dy in order:
            _, _, y, c = p.at(0, 0, dy, 1)
            cores[k, dy] = push(g_ref.at[y * 2 + c, part[k]], rc.at[dy, part[k]], (0, 0, 0, 1))

    def first():
        for k in range(pieces):
            for dy in order:
                _, _, y, c = p.at(0, 0, dy, 0)
                cores[k, dy].wait_recv()
                both = g_ref[y * 2 + c, part[k], :].astype(jnp.float32) + rc[dy, part[k], :].astype(jnp.float32)
                if dy:
                    acc[dy - 1, part[k], :] = both.astype(acc.dtype)
                    along[k, dy] = push(acc.at[dy - 1, part[k]], ry.at[dy - 1, part[k]], (0, 0, dy, 0))
                else:
                    out_ref[part[k], :] = both

    def second():
        for k in range(pieces):
            for dy in range(1, ny):
                along[k, dy].wait_recv()
                out_ref[part[k], :] = out_ref[part[k], :] + ry[dy - 1, part[k], :].astype(jnp.float32)

    return first, second


def pack_reduce_kernel(g_ref, out_ref, acc, rc, ry, send, recv):
    p = Place()
    p.greet([(0, 0, d, 0) for d in range(1, p.ny)] + [(0, 0, 0, 1)])
    s, r = Pool(send), Pool(recv)
    sent = []

    def push(src, dst, to):
        cp = pltpu.make_async_remote_copy(src_ref=src, dst_ref=dst, send_sem=s.take(), recv_sem=r.take(),
            device_id=p.dev(*to), device_id_type=MESH)
        cp.start()
        sent.append(cp)
        return cp

    first, second = pack_reduce_body(p, g_ref, out_ref, acc, rc, ry, push)
    first()
    second()
    for cp in sent:
        cp.wait_send()


def pack_scratch(ny, rows, width, dt):
    return [pltpu.VMEM((ny - 1, rows, width), dt), pltpu.VMEM((ny, rows, width), dt), pltpu.VMEM((ny - 1, rows, width), dt)]


def pack_reduce(terms, cid):
    nz, nx, ny = grid_of()
    ns, rows, width = terms.shape
    n = 8 * ny
    return pl.pallas_call(pack_reduce_kernel,
        out_shape=jax.ShapeDtypeStruct((rows, width), jnp.float32), in_specs=[VM], out_specs=VM,
        scratch_shapes=pack_scratch(ny, rows, width, terms.dtype)
            + [pltpu.SemaphoreType.DMA((n,)), pltpu.SemaphoreType.DMA((n,))],
        compiler_params=pltpu.CompilerParams(collective_id=cid, has_side_effects=True, vmem_limit_bytes=40 << 20),
        name="pack_reduce")(terms)


def grads_kernel(wo_ref, w_ref, s_ref, n_ref, wo_out, w_out, s_out, n_out,
                 wo_x, wo_z, wo_l, wo_r, w_x, w_z, w_l, w_r, s_x, s_z, s_l, acc, rc, ry, load_sem, send, recv):
    p = Place()
    nz, nx, ny = p.nz, p.nx, p.ny
    ns, ne = ny * 2, nz * nx
    e, sh = lax.axis_index("expert"), lax.axis_index("shard")
    me = e * ns + sh
    own_e, own_s = (sh * ne + e) // ns, (sh * ne + e) % ns
    from_e, from_s = me % ne, me // ne
    moved = jnp.logical_not(jnp.logical_and(own_e == e, own_s == sh))
    peers = [q for q in p.line_peers() if not (q[2] or q[3])] + shard_peers(ny)
    barrier = pltpu.get_barrier_semaphore()
    for q in peers:
        pl.semaphore_signal(barrier, inc=1, device_id=p.dev(*q), device_id_type=MESH)

    @pl.when(moved)
    def _():
        pl.semaphore_signal(barrier, inc=1, device_id=(from_e, from_s), device_id_type=MESH)

    pl.semaphore_wait(barrier, len(peers) + moved.astype(jnp.int32))
    s, r = Pool(send), Pool(recv)
    sent = []

    def push(src, dst, to):
        cp = pltpu.make_async_remote_copy(src_ref=src, dst_ref=dst, send_sem=s.take(), recv_sem=r.take(),
            device_id=p.dev(*to), device_id_type=MESH)
        cp.start()
        sent.append(cp)
        return cp

    zs = list(range(1, nz)) + [0]
    jobs = [(w_ref, w_x, w_z, w_l, ns, 0), (s_ref, s_x, s_z, s_l, ns, nz), (wo_ref, wo_x, wo_z, wo_l, 1, 2 * nz)]

    def group(ref, dz, dx, size):
        z, x, _, _ = p.at(dz, dx, 0, 0)
        return ref.at[pl.ds((z * nx + x) * size, size)]

    xs, loads, lines = {}, {}, {}
    for j, (ref, x_buf, z_buf, l_buf, size, base) in enumerate(jobs):
        for dz in zs:
            for dx in range(1, nx):
                xs[j, dz, dx] = push(group(ref, dz, dx, size), x_buf.at[dx - 1, dz], (0, dx, 0, 0))
            loads[j, dz] = pltpu.make_async_copy(group(ref, dz, 0, size), l_buf.at[dz], load_sem.at[base + dz])
            loads[j, dz].start()
    first, second = pack_reduce_body(p, n_ref, n_out, acc, rc, ry, push)
    first()
    for j, (ref, x_buf, z_buf, l_buf, size, base) in enumerate(jobs):
        for dz in zs:
            loads[j, dz].wait()
            for dx in range(1, nx):
                xs[j, dz, dx].wait_recv()
            total = l_buf[dz].astype(jnp.float32)
            for dx in range(1, nx):
                total = total + x_buf[dx - 1, dz].astype(jnp.float32)
            l_buf[dz] = total.astype(l_buf.dtype)
            if dz:
                lines[j, dz] = push(l_buf.at[dz], z_buf.at[dz - 1], (dz, 0, 0, 0))
    second()
    last = []
    entry = pltpu.make_async_remote_copy(src_ref=wo_l.at[0, 0], dst_ref=wo_r, send_sem=s.take(),
        recv_sem=r.take(), device_id=(own_e, own_s), device_id_type=MESH)
    for j, (ref, x_buf, z_buf, l_buf, size, base) in enumerate(jobs):
        total = l_buf[0].astype(jnp.float32)
        for d in range(1, nz):
            lines[j, d].wait_recv()
            total = total + z_buf[d - 1].astype(jnp.float32)
        l_buf[0] = total.astype(l_buf.dtype)
        if j == 0:
            for q in shard_peers(ny):
                _, _, y, c = p.at(*q)
                last.append(push(l_buf.at[0, y * 2 + c], w_r.at[sh], q))
            w_r[sh] = l_buf[0, sh]
        elif j == 1:
            for q in shard_peers(ny):
                _, _, y, c = p.at(*q)
                last.append(push(l_buf.at[0, y * 2 + c], s_out.at[sh], q))
            s_out[sh] = l_buf[0, sh]

    @pl.when(moved)
    def _():
        entry.start()

    for cp in last:
        cp.wait_recv()
    w_out[...] = w_r[...].astype(jnp.float32)

    @pl.when(moved)
    def _():
        entry.wait()
        wo_out[...] = wo_r[...].astype(jnp.float32)

    @pl.when(jnp.logical_not(moved))
    def _():
        wo_out[...] = wo_l[0, 0].astype(jnp.float32)

    for cp in sent:
        cp.wait_send()


def reduce_grads(wo, w, small, inp, cid):
    nz, nx, ny = grid_of()
    ns, ne = ny * 2, nz * nx
    bf, f32 = jnp.bfloat16, jnp.float32
    rows_o, width = wo.shape[1:]
    rows_w, cb = w.shape[1:]
    rows_n = inp.shape[1]
    n = 3 * nz * nx + 3 * nz + 2 * ns + 8 * ny + 8
    small_block = small.shape[1:]
    return pl.pallas_call(grads_kernel,
        out_shape=(jax.ShapeDtypeStruct((rows_o, width), f32), jax.ShapeDtypeStruct((ns, rows_w, cb), f32),
            jax.ShapeDtypeStruct((ns,) + small_block, f32), jax.ShapeDtypeStruct((rows_n, width), f32)),
        in_specs=[ANY, ANY, ANY, VM], out_specs=(VM, VM, VM, VM),
        scratch_shapes=[pltpu.VMEM((nx - 1, nz, 1, rows_o, width), bf), pltpu.VMEM((nz - 1, 1, rows_o, width), bf),
            pltpu.VMEM((nz, 1, rows_o, width), bf), pltpu.VMEM((rows_o, width), bf),
            pltpu.VMEM((nx - 1, nz, ns, rows_w, cb), bf), pltpu.VMEM((nz - 1, ns, rows_w, cb), bf),
            pltpu.VMEM((nz, ns, rows_w, cb), bf), pltpu.VMEM((ns, rows_w, cb), bf),
            pltpu.VMEM((nx - 1, nz, ns) + small_block, f32), pltpu.VMEM((nz - 1, ns) + small_block, f32),
            pltpu.VMEM((nz, ns) + small_block, f32)]
            + pack_scratch(ny, rows_n, width, bf)
            + [pltpu.SemaphoreType.DMA((3 * nz,)), pltpu.SemaphoreType.DMA((n,)), pltpu.SemaphoreType.DMA((n,))],
        compiler_params=pltpu.CompilerParams(collective_id=cid, has_side_effects=True, vmem_limit_bytes=56 << 20),
        name="reduce_grads")(wo, w, small, inp)


QUERY_HEADS = 32
KEY_VALUE_HEADS = 4
HEAD = 128
EPSILON = 1e-06
THETA = 1000000.0


def norm_rows(values_in, gain):
    return values_in * lax.rsqrt(jnp.mean(values_in * values_in, axis=-1, keepdims=True) + EPSILON) * gain


def rotate(vectors, position):
    half_size = vectors.shape[-1] // 2
    freqs = jnp.exp(jnp.arange(half_size, dtype=jnp.float32) * (-2.0 * math.log(THETA) / vectors.shape[-1]))
    angles = position[:, None] * freqs[None, :]
    cosine = jnp.cos(angles)[:, None, :]
    sine = jnp.sin(angles)[:, None, :]
    first = vectors[..., :half_size]
    second = vectors[..., half_size:]
    return jnp.concatenate([first * cosine - second * sine, second * cosine + first * sine], axis=-1)


def segment_starts(segment):
    index = jnp.arange(segment.shape[0], dtype=jnp.int32)
    same = segment[:, None] == segment[None, :]
    return jnp.min(jnp.where(same, index[None, :], segment.shape[0]), axis=1)


def shards(tokens_in, out_grad, segment_ids, expert_ids, route_weights, attn_gain, qkv_weight, q_gain, k_gain,
           out_weight, moe_gain, expert_in, expert_out):
    f32, bf = jnp.float32, jnp.bfloat16
    n_expert, n_shard = lax.axis_size("expert"), lax.axis_size("shard")
    nd = n_expert * n_shard
    rows, width = tokens_in.shape
    me = lax.axis_index("expert") * n_shard + lax.axis_index("shard")
    shard = lax.axis_index("shard")
    heads = QUERY_HEADS // n_shard
    group = QUERY_HEADS // KEY_VALUE_HEADS
    kv_heads = max(1, KEY_VALUE_HEADS // n_shard)
    copies = max(1, n_shard // KEY_VALUE_HEADS)
    per = heads // kv_heads
    q_cols, kv_cols = heads * HEAD, kv_heads * HEAD
    q_all, kv_all = QUERY_HEADS * HEAD, KEY_VALUE_HEADS * HEAD
    wide = qkv_weight.shape[0]

    scaled = (qkv_weight.astype(f32) * attn_gain.astype(f32)[:, None]).astype(bf)

    def by_shard(part, cols, count):
        part = part.reshape(wide, n_shard // count, 1, cols)
        return jnp.broadcast_to(part, (wide, n_shard // count, count, cols)).reshape(wide, n_shard, cols)

    pieces = jnp.concatenate([by_shard(scaled[:, :q_all], q_cols, 1),
        by_shard(scaled[:, q_all:q_all + kv_all], kv_cols, copies),
        by_shard(scaled[:, q_all + kv_all:], kv_cols, copies)], axis=2).transpose(1, 0, 2)
    weights, out_rows, pack = gather_weights(pieces, out_weight, tokens_in, 0)
    weights = weights.reshape(width, -1)
    out_rows = out_rows.reshape(heads * HEAD, width)
    pack = pack.reshape(n_shard * rows, width)
    length = pack.shape[0]

    high = route_weights.astype(bf)
    rest = route_weights - high.astype(f32)
    middle = rest.astype(bf)
    low = (rest - middle.astype(f32)).astype(bf)
    top = expert_ids.shape[1]
    gains = jnp.zeros((rows,), bf)
    at = 0
    for g in (moe_gain, q_gain, k_gain):
        gains = lax.dynamic_update_slice(gains, g, (at,))
        at += g.shape[0]
    extra = jnp.concatenate([expert_ids.astype(bf), high, middle, low, gains[:, None]], axis=1)
    extra = jnp.pad(extra, ((0, 0), (0, 128 - extra.shape[1])))
    grads_all = gather_all(jnp.concatenate([out_grad, extra], axis=1), 1)
    info = grads_all[:, :, width:].astype(f32)
    ids_all = info[:, :, :top]
    weights_all = info[:, :, top:2 * top] + info[:, :, 2 * top:3 * top] + info[:, :, 3 * top:4 * top]
    gain_col = info[:, :, 4 * top]
    g0, g1, g2 = moe_gain.shape[0], q_gain.shape[0], k_gain.shape[0]
    moe_scale = gain_col[:, :g0].reshape(-1)
    query_gain = gain_col[:, g0:g0 + g1].reshape(-1)
    key_gain = gain_col[:, g0 + g1:g0 + g1 + g2].reshape(-1)

    pack_f32 = pack.astype(f32)
    inverse = lax.rsqrt(jnp.mean(pack_f32 * pack_f32, axis=-1, keepdims=True) + EPSILON)
    projected = jnp.dot(pack, weights, preferred_element_type=f32) * inverse
    segment = segment_ids[0]
    index = jnp.arange(length, dtype=jnp.int32)
    position = (index - segment_starts(segment)).astype(f32)
    query_raw = projected[:, :q_cols].reshape(length, heads, HEAD)
    key_raw = projected[:, q_cols:q_cols + kv_cols].reshape(length, kv_heads, HEAD)
    values = projected[:, q_cols + kv_cols:].astype(bf).reshape(length, kv_heads, HEAD)

    def prepare(query_in, key_in, gain_q, gain_k):
        return rotate(norm_rows(query_in, gain_q), position), rotate(norm_rows(key_in, gain_k), position)

    (query_rot, key_rot), prepare_back = jax.vjp(prepare, query_raw, key_raw, query_gain, key_gain)
    queries = query_rot.astype(bf).reshape(length, kv_heads, per, HEAD)
    keys = key_rot.astype(bf)
    allowed = (segment[:, None] == segment[None, :]) & (index[None, :] <= index[:, None])
    factor = HEAD ** (-0.5)
    scores = jnp.einsum("tkgd,skd->kgts", queries, keys, preferred_element_type=f32) * factor
    scores = jnp.where(allowed[None, None], scores, -1e30)
    highest = jnp.max(scores, axis=-1, keepdims=True)
    log_total = highest + jnp.log(jnp.sum(jnp.exp(scores - highest), axis=-1, keepdims=True))
    probs = jnp.exp(scores - log_total)
    probs_low = probs.astype(bf)
    attn = jnp.einsum("kgts,skd->tkgd", probs_low, values, preferred_element_type=f32).astype(bf)
    attn_flat = attn.reshape(length, q_cols)
    mixed = jnp.dot(attn_flat, out_rows, preferred_element_type=f32).astype(bf)
    hidden_state = tokens_in.astype(f32) + pack_reduce(mixed.reshape(n_shard, rows, width), 2)
    hidden_inverse = lax.rsqrt(jnp.mean(hidden_state * hidden_state, axis=-1, keepdims=True) + EPSILON)
    hidden_norm = hidden_state * hidden_inverse
    moe_in = (hidden_norm * moe_scale).astype(bf)

    rows_all = gather_all(moe_in, 3)
    cap = max(2, 2 * rows * top // nd)
    hit = ids_all == me.astype(f32)
    any_hit = jnp.any(hit, axis=-1)
    gate = jnp.sum(jnp.where(hit, weights_all, 0.0), axis=-1)
    lower = (jnp.arange(rows)[:, None] <= jnp.arange(rows)[None, :]).astype(bf)
    rank = jnp.dot(any_hit.astype(bf), lower, preferred_element_type=f32) - 1.0
    chosen = (jnp.arange(cap, dtype=f32)[None, :, None] == rank[:, None, :]) & any_hit[:, None, :]
    slot_gate = jnp.sum(jnp.where(chosen, gate[:, None, :], 0.0), axis=-1)
    select = chosen.astype(bf)
    in_rows = jnp.einsum("bkt,btd->bkd", select, rows_all, preferred_element_type=f32).astype(bf).reshape(nd * cap, width)
    grad_rows = (jnp.einsum("bkt,btd->bkd", select, grads_all[:, :, :width], preferred_element_type=f32)
        * slot_gate[:, :, None]).astype(bf).reshape(nd * cap, width)
    w_in, w_out = expert_in[0], expert_out[0]
    size = w_out.shape[0]
    pre = jnp.dot(in_rows, w_in, preferred_element_type=f32)
    gate_part, up_part = pre[:, :size], pre[:, size:]
    sigma = jax.nn.sigmoid(gate_part)
    active = gate_part * sigma
    hidden = (active * up_part).astype(bf)
    outputs = jnp.dot(hidden, w_out, preferred_element_type=f32).astype(bf)
    weighted = (outputs.astype(f32) * slot_gate.reshape(-1, 1)).astype(bf).reshape(nd, cap, width)
    out_terms = jnp.einsum("bkt,bkd->btd", select, weighted, preferred_element_type=f32).astype(bf)
    moe_sum = reduce_all(out_terms, f32, 4)
    hidden_grad = jnp.einsum("rd,fd->rf", grad_rows, w_out, preferred_element_type=f32)
    gate_grad = hidden_grad * up_part * (sigma * (1.0 + gate_part * (1.0 - sigma)))
    pre_grad = jnp.concatenate([gate_grad, hidden_grad * active], axis=-1).astype(bf)
    rows_grad = jnp.einsum("rc,dc->rd", pre_grad, w_in, preferred_element_type=f32).astype(bf).reshape(nd, cap, width)
    grad_terms = jnp.einsum("bkt,bkd->btd", select, rows_grad, preferred_element_type=f32).astype(bf)
    moe_grad = reduce_all(grad_terms, f32, 5)
    expert_in_grad = jnp.einsum("rd,rc->dc", in_rows, pre_grad, preferred_element_type=f32)[None]
    expert_out_grad = jnp.einsum("rf,rd->fd", hidden, grad_rows, preferred_element_type=f32)[None]
    block_output = (hidden_state + moe_sum).astype(bf)

    scaled_grad = moe_grad * moe_scale
    moe_gain_grad = jnp.sum(moe_grad * hidden_norm, axis=0)
    residual = out_grad.astype(f32) + hidden_inverse * (
        scaled_grad - hidden_norm * jnp.mean(scaled_grad * hidden_norm, axis=-1, keepdims=True))
    residual_pack = pack_gather(residual.astype(bf), 6).reshape(length, width)
    out_term = jnp.einsum("tc,td->cd", attn_flat, residual_pack, preferred_element_type=f32).astype(bf)
    attn_grad = jnp.einsum("td,cd->tc", residual_pack, out_rows, preferred_element_type=f32).astype(bf)
    attn_grad = attn_grad.reshape(length, kv_heads, per, HEAD)
    delta = jnp.einsum("tkgd,tkgd->kgt", attn_grad, attn, preferred_element_type=f32)
    prob_grad = jnp.einsum("tkgd,skd->kgts", attn_grad, values, preferred_element_type=f32)
    score_grad = (probs * (prob_grad - delta[..., None])).astype(bf)
    query_grad = jnp.einsum("kgts,skd->tkgd", score_grad, keys, preferred_element_type=f32) * factor
    key_grad = jnp.einsum("kgts,tkgd->skd", score_grad, queries, preferred_element_type=f32) * factor
    value_grad = jnp.einsum("kgts,tkgd->skd", probs_low, attn_grad, preferred_element_type=f32)
    query_back, key_back, query_gain_grad, key_gain_grad = prepare_back((query_grad.reshape(length, heads, HEAD), key_grad))
    projected_grad = jnp.concatenate([query_back.reshape(length, -1), key_back.reshape(length, -1),
        value_grad.reshape(length, -1)], axis=1)
    projected_grad = (projected_grad * inverse).astype(bf)
    qkv_term = jnp.einsum("td,tc->dc", pack, projected_grad, preferred_element_type=f32).astype(bf)
    input_term = jnp.einsum("tc,dc->td", projected_grad, weights, preferred_element_type=f32).astype(bf)

    def lanes(v):
        v = v.reshape(nd, -1)
        return jnp.pad(v, ((0, 0), (0, 128 - v.shape[1])))[:, None]

    small = jnp.concatenate([lanes(moe_gain_grad), lanes(query_gain_grad), lanes(key_gain_grad),
        jnp.zeros((nd, 5, 128), f32)], axis=1)
    out_weight_grad, qkv_part, small_sum, input_sum = reduce_grads(out_term.reshape(n_expert, -1, width),
        qkv_term.reshape(nd, wide, -1), small, input_term.reshape(n_shard, rows, width), 7)
    small_sum = jnp.sum(small_sum, axis=0)

    def whole_cols(part, count):
        part = part.transpose(1, 0, 2).reshape(wide, n_shard // count, count, -1)
        return jnp.sum(part, axis=2).reshape(wide, -1)

    raw = jnp.concatenate([whole_cols(qkv_part[:, :, :q_cols], 1), whole_cols(qkv_part[:, :, q_cols:q_cols + kv_cols], copies),
        whole_cols(qkv_part[:, :, q_cols + kv_cols:], copies)], axis=1)
    attn_gain_grad = jnp.sum(raw * qkv_weight.astype(f32), axis=1)
    qkv_weight_grad = raw * attn_gain.astype(f32)[:, None]
    own = tokens_in.astype(f32)
    own_norm = own * lax.rsqrt(jnp.mean(own * own, axis=-1, keepdims=True) + EPSILON)
    input_grad = (residual + input_sum - own_norm * jnp.mean(input_sum * own_norm, axis=-1, keepdims=True)).astype(bf)
    return (block_output, input_grad, attn_gain_grad, qkv_weight_grad, small_sum[1, :g1], small_sum[2, :g2],
        out_weight_grad, small_sum[0, :g0], expert_in_grad, expert_out_grad)


def solution(mesh):
    both = ("expert", "shard")
    row, rows2, rows3 = P(both), P(both, None), P(both, None, None)
    return jax.shard_map(
        shards, mesh=mesh,
        in_specs=(rows2, rows2, P("expert", None), rows2, rows2, row, rows2, row, row, rows2, row, rows3, rows3),
        out_specs=(rows2, rows2, row, rows2, row, row, rows2, row, rows3, rows3),
        check_vma=False,
    )
```

```python
import functools
import math
import jax, jax.numpy as jnp
from jax import lax
from jax.experimental import pallas as pl
from jax.experimental.pallas import tpu as pltpu
from jax.sharding import PartitionSpec as P
MESH = pl.DeviceIdType.MESH
ANY = pl.BlockSpec(memory_space=pl.ANY)
VM = pl.BlockSpec(memory_space=pltpu.VMEM)

def grid_of():
    n_expert, n_shard = lax.axis_size("expert"), lax.axis_size("shard")
    ny = n_shard // 2
    nx = min(ny, n_expert)
    return n_expert // nx, nx, ny

class Place:
    def __init__(self):
        self.nz, self.nx, self.ny = grid_of()
        e, s = lax.axis_index("expert"), lax.axis_index("shard")
        self.z, self.x = e // self.nx, e % self.nx
        self.y, self.c = s // 2, s % 2
    def dev(self, dz=0, dx=0, dy=0, dc=0):
        z, x, y, c = self.at(dz, dx, dy, dc)
        return (z * self.nx + x, y * 2 + c)
    def at(self, dz=0, dx=0, dy=0, dc=0):
        z = lax.rem(self.z + dz + self.nz, self.nz) if dz else self.z
        x = lax.rem(self.x + dx + self.nx, self.nx) if dx else self.x
        y = lax.rem(self.y + dy + self.ny, self.ny) if dy else self.y
        c = 1 - self.c if dc else self.c
        return z, x, y, c
    def index(self, dz=0, dx=0, dy=0, dc=0):
        z, x, y, c = self.at(dz, dx, dy, dc)
        return ((z * self.nx + x) * self.ny + y) * 2 + c
    def greet(self, peers):
        barrier = pltpu.get_barrier_semaphore()
        for p in peers:
            pl.semaphore_signal(barrier, inc=1, device_id=self.dev(*p), device_id_type=MESH)
        pl.semaphore_wait(barrier, len(peers))
    def line_peers(self):
        return ([(d, 0, 0, 0) for d in range(1, self.nz)] + [(0, d, 0, 0) for d in range(1, self.nx)]
                + [(0, 0, d, 0) for d in range(1, self.ny)] + [(0, 0, 0, 1)])

class Pool:
    def __init__(self, sems):
        self.sems, self.used = sems, 0
    def take(self):
        self.used += 1
        return self.sems.at[self.used - 1]

def n_sems(nz, nx, ny):
    return (nz - 1) + nz * (nx - 1 + ny - 1 + 1) + nz * (nx * (ny - 1) + ny * (nx - 1)) + nz * (nx - 1 + ny - 1) + nz * (nx * (ny - 1) + ny * (nx - 1))

def reduce_rows_kernel(g_ref, selt_ref, out_ref, give, acc, rc, ra1, rb1, ra2, rb2, rz, send, recv):
    p = Place()
    nz, nx, ny = p.nz, p.nx, p.ny
    rows = selt_ref.shape[1]
    half = rows // 2
    f32 = jnp.float32
    A, B = pl.ds(0, half), pl.ds(half, half)
    p.greet(p.line_peers())
    s, r = Pool(send), Pool(recv)
    sent = []
    slot = lambda dz, dx, dy: (dz * nx + dx) * ny + dy

    def push(src, dst, to):
        cp = pltpu.make_async_remote_copy(src_ref=src, dst_ref=dst, send_sem=s.take(), recv_sem=r.take(),
            device_id=p.dev(*to), device_id_type=MESH)
        cp.start()
        sent.append(cp)
        return cp

    zs = list(range(1, nz)) + [0]
    plane = [(dx, dy) for dx in reversed(range(nx)) for dy in reversed(range(ny))]
    cores, ca, cb, za, zb, zz = {}, {}, {}, {}, {}, {}

    def term(i):
        return jnp.dot(selt_ref[i], g_ref[i], preferred_element_type=f32)

    def stage_zero(dz):
        for dx, dy in plane:
            k = (dz, dx, dy)
            i = slot(*k)
            give[i] = term(p.index(*k, 1)).astype(give.dtype)
            cores[k] = push(give.at[i], rc.at[i], (0, 0, 0, 1))

    def add(dst, rows_, src):
        acc[dst, rows_, :] = (acc[dst, rows_, :].astype(f32) + src[...].astype(f32)).astype(acc.dtype)

    def stage_one(dz):
        for dx, dy in plane:
            k = (dz, dx, dy)
            i = slot(*k)
            mine = term(p.index(*k))
            cores[k].wait_recv()
            acc[i] = (mine + rc[i].astype(f32)).astype(acc.dtype)
            if dy:
                ca[k] = push(acc.at[i, A], ra1.at[dy - 1, dz * nx + dx], (0, 0, dy, 0))
            if dx:
                cb[k] = push(acc.at[i, B], rb1.at[dx - 1, dz * ny + dy], (0, dx, 0, 0))

    def stage_two(dz):
        for dx in reversed(range(nx)):
            for dy in range(1, ny):
                ca[dz, dx, dy].wait_recv()
                add(slot(dz, dx, 0), A, ra1.at[dy - 1, dz * nx + dx])
            if dx:
                za[dz, dx] = push(acc.at[slot(dz, dx, 0), A], ra2.at[dx - 1, dz], (0, dx, 0, 0))
        for dy in reversed(range(ny)):
            for dx in range(1, nx):
                cb[dz, dx, dy].wait_recv()
                add(slot(dz, 0, dy), B, rb1.at[dx - 1, dz * ny + dy])
            if dy:
                zb[dz, dy] = push(acc.at[slot(dz, 0, dy), B], rb2.at[dy - 1, dz], (0, 0, dy, 0))

    def stage_three(dz):
        for dx in range(1, nx):
            za[dz, dx].wait_recv()
            add(slot(dz, 0, 0), A, ra2.at[dx - 1, dz])
        for dy in range(1, ny):
            zb[dz, dy].wait_recv()
            add(slot(dz, 0, 0), B, rb2.at[dy - 1, dz])
        if dz:
            zz[dz] = push(acc.at[slot(dz, 0, 0)], rz.at[dz - 1], (dz, 0, 0, 0))

    stage_zero(zs[0])
    for k in range(nz + 2):
        if k + 1 < nz:
            stage_zero(zs[k + 1])
        if k < nz:
            stage_one(zs[k])
        if 0 <= k - 1 < nz:
            stage_two(zs[k - 1])
        if 0 <= k - 2 < nz:
            stage_three(zs[k - 2])
    total = acc[slot(0, 0, 0)].astype(f32)
    for dz in range(1, nz):
        zz[dz].wait_recv()
        total = total + rz[dz - 1].astype(f32)
    out_ref[...] = total
    for cp in sent:
        cp.wait_send()


def reduce_rows(made, select, cid):
    nz, nx, ny = grid_of()
    nd, cap, width = made.shape
    rows = select.shape[2]
    dt = made.dtype
    half = rows // 2
    n = 3 * nz * nx * ny + nz * (nx + ny) + nz
    blocks = 3 * nz * nx * ny + nz + (nz * (nx + 1) * (ny - 1) + nz * (ny + 1) * (nx - 1)) // 2 + 4
    parts = 1
    while (blocks * rows + nd * cap) * width * 2 // parts > 50 << 20:
        parts *= 2
    cols = width // parts
    one = pl.pallas_call(reduce_rows_kernel,
        out_shape=jax.ShapeDtypeStruct((rows, cols), jnp.float32),
        in_specs=[VM, VM], out_specs=VM,
        scratch_shapes=[pltpu.VMEM((nz * nx * ny, rows, cols), dt), pltpu.VMEM((nz * nx * ny, rows, cols), dt),
            pltpu.VMEM((nz * nx * ny, rows, cols), dt),
            pltpu.VMEM((ny - 1, nz * nx, half, cols), dt), pltpu.VMEM((nx - 1, nz * ny, half, cols), dt),
            pltpu.VMEM((nx - 1, nz, half, cols), dt), pltpu.VMEM((ny - 1, nz, half, cols), dt),
            pltpu.VMEM((nz - 1, rows, cols), dt),
            pltpu.SemaphoreType.DMA((n,)), pltpu.SemaphoreType.DMA((n,))],
        compiler_params=pltpu.CompilerParams(collective_id=cid, has_side_effects=True, vmem_limit_bytes=61 << 20),
        name="reduce_rows")
    turned = select.transpose(0, 2, 1)
    if parts == 1:
        return one(made, turned)
    return jnp.concatenate([one(made[:, :, k * cols:(k + 1) * cols], turned) for k in range(parts)], axis=1)


def expert_kernel(b_ref, sel_ref, selt_ref, gate_ref, g_ref, win_ref, wout_ref,
                  all_ref, in_ref, gr_ref, hid_ref, pg_ref, out_ref, back_ref,
                  xt, gt, in_t, gr_t, hid_t, pg_t, out_t, back_t, local_sem, x_sem, g_sem, store_sem, send, recv):
    p = Place()
    nz, nx, ny = p.nz, p.nx, p.ny
    ns = 2 * ny
    half = b_ref.shape[0] // 2
    cap = sel_ref.shape[1]
    size, width = wout_ref.shape
    f32, bf = jnp.float32, jnp.bfloat16
    A, B = pl.ds(0, half), pl.ds(half, half)
    F = pl.ds(0, 2 * half)
    p.greet(p.line_peers())
    own = pltpu.make_async_copy(b_ref, all_ref.at[p.index()], local_sem)
    own.start()
    s, r = Pool(send), Pool(recv)
    sent = []
    neg = lambda d, n: (n - d) % n

    def push(src_at, rows, to, first=False):
        i = p.index(*src_at)
        src = b_ref.at[rows] if first else all_ref.at[i, rows]
        cp = pltpu.make_async_remote_copy(src_ref=src, dst_ref=all_ref.at[i, rows], send_sem=s.take(),
            recv_sem=r.take(), device_id=p.dev(*to), device_id_type=MESH)
        cp.start()
        sent.append(cp)
        return cp

    first = {d: push((0, 0, 0, 0), F, (d, 0, 0, 0), True) for d in range(1, nz)}
    second_a, second_b, third, other = {}, {}, {}, {}

    def cross(at, rows, is_first=False):
        dx = neg(at[1], nx)
        other.setdefault((neg(at[0], nz), dx), []).append(push(at, rows, (0, 0, 0, 1), is_first))

    def stage_one(k):
        if k:
            first[k].wait_recv()
        at = (neg(k, nz), 0, 0, 0)
        for d in range(1, nx):
            second_a[k, d] = push(at, A, (0, d, 0, 0), k == 0)
        for d in range(1, ny):
            second_b[k, d] = push(at, B, (0, 0, d, 0), k == 0)
        for d in range(1, ny):
            third["a", k, 0, d] = push(at, A, (0, 0, d, 0), k == 0)
        for d in range(1, nx):
            third["b", k, 0, d] = push(at, B, (0, d, 0, 0), k == 0)
        cross(at, F, k == 0)

    def stage_two(k):
        for dx in range(1, nx):
            second_a[k, dx].wait_recv()
            at = (neg(k, nz), neg(dx, nx), 0, 0)
            for d in range(1, ny):
                third["a", k, dx, d] = push(at, A, (0, 0, d, 0))
            cross(at, A)
        for dy in range(1, ny):
            second_b[k, dy].wait_recv()
            at = (neg(k, nz), 0, neg(dy, ny), 0)
            for d in range(1, nx):
                third["b", k, dy, d] = push(at, B, (0, d, 0, 0))
            cross(at, B)

    def stage_three(k):
        for dx in range(nx):
            for d in range(1, ny):
                third["a", k, dx, d].wait_recv()
                cross((neg(k, nz), neg(dx, nx), neg(d, ny), 0), A)
        for dy in range(ny):
            for d in range(1, nx):
                third["b", k, dy, d].wait_recv()
                cross((neg(k, nz), neg(d, nx), neg(dy, ny), 0), B)

    whole = nx * ns <= 8
    groups = [(k, None) for k in range(nz)] if whole else [(k, dx) for k in range(nz) for dx in range(nx)]
    gb = nx * ns if whole else ns

    def base_of(i):
        k, dx = groups[i]
        z, x, _, _ = p.at(neg(k, nz), neg(dx or 0, nx), 0, 0)
        return z * nx * ns if whole else (z * nx + x) * ns

    def load_x(i):
        return pltpu.make_async_copy(all_ref.at[pl.ds(base_of(i), gb)], xt, x_sem)

    def load_g(i):
        return pltpu.make_async_copy(g_ref.at[pl.ds(base_of(i), gb)], gt.at[i % 2], g_sem.at[i % 2])

    def stores(i, part):
        rows = pl.ds(base_of(i) * cap, gb * cap)
        pairs = [[(in_t, in_ref.at[rows]), (gr_t, gr_ref.at[rows])], [(hid_t, hid_ref.at[rows]), (pg_t, pg_ref.at[rows])],
            [(out_t, out_ref.at[pl.ds(base_of(i), gb)]), (back_t, back_ref.at[rows])]][part]
        return [pltpu.make_async_copy(a, b, store_sem.at[part, j]) for j, (a, b) in enumerate(pairs)]

    def compute(i):
        load_x(i).start()
        if i + 1 < len(groups):
            load_g(i + 1).start()
        load_g(i).wait()
        base = base_of(i)
        if i:
            for cp in stores(i - 1, 0):
                cp.wait()
        load_x(i).wait()

        def pick(b, carry):
            rows = pl.ds(pl.multiple_of(b * cap, cap), cap)
            sel = sel_ref[base + b]
            in_t[rows, :] = jnp.dot(sel, xt[b], preferred_element_type=f32).astype(bf)
            gr_t[rows, :] = (jnp.dot(sel, gt[i % 2, b], preferred_element_type=f32) * gate_ref[base + b][:, :1]).astype(bf)
            return carry

        lax.fori_loop(0, gb, pick, 0)
        for cp in stores(i, 0):
            cp.start()
        if i:
            for cp in stores(i - 1, 1):
                cp.wait()
        wide = min(size, 256)

        def middle(j, carry):
            left = pl.ds(pl.multiple_of(j * wide, wide), wide)
            right = pl.ds(pl.multiple_of(size + j * wide, wide), wide)
            rows_in, rows_grad = in_t[...], gr_t[...]
            a = jnp.dot(rows_in, win_ref[:, left], preferred_element_type=f32)
            b = jnp.dot(rows_in, win_ref[:, right], preferred_element_type=f32)
            h = lax.dot_general(rows_grad, wout_ref[left, :], (((1,), (1,)), ((), ())), preferred_element_type=f32)
            sigma = 1.0 / (1.0 + jnp.exp(-a))
            active = a * sigma
            hid_t[:, left] = (active * b).astype(bf)
            pg_t[:, left] = (h * b * (sigma * (1.0 + a * (1.0 - sigma)))).astype(bf)
            pg_t[:, right] = (h * active).astype(bf)
            return carry

        lax.fori_loop(0, size // wide, middle, 0)
        for cp in stores(i, 1):
            cp.start()
        if i:
            for cp in stores(i - 1, 2):
                cp.wait()
        gates = jnp.concatenate([gate_ref[base + b][:, :1] for b in range(gb)], axis=0)

        def final(j, carry):
            cols = pl.ds(pl.multiple_of(j * 256, 256), 256)
            out = jnp.dot(hid_t[...], wout_ref[:, cols], preferred_element_type=f32).astype(bf)
            weighted = (out.astype(f32) * gates).astype(bf)
            back_t[:, cols] = lax.dot_general(pg_t[...], win_ref[cols, :], (((1,), (1,)), ((), ())),
                preferred_element_type=f32).astype(bf)
            for b in range(gb):
                out_t[b, :, cols] = jnp.dot(selt_ref[base + b], weighted[b * cap:(b + 1) * cap],
                    preferred_element_type=f32).astype(bf)
            return carry

        lax.fori_loop(0, width // 256, final, 0)
        for cp in stores(i, 2):
            cp.start()

    load_g(0).start()
    for k in range(nz + 2):
        if k < nz:
            stage_one(k)
        if 0 <= k - 1 < nz:
            stage_two(k - 1)
        if 0 <= k - 2 < nz:
            stage_three(k - 2)
            if k == 2:
                own.wait()
            for i, (z_group, dx) in enumerate(groups):
                if z_group == k - 2:
                    for each in (range(nx) if whole else [dx]):
                        for cp in other[k - 2, each]:
                            cp.wait_recv()
                    compute(i)
    for part in range(3):
        for cp in stores(len(groups) - 1, part):
            cp.wait()
    for cp in sent:
        cp.wait_send()


def expert_pass(block, select, gate, grads_all, w_in, w_out, cid):
    nz, nx, ny = grid_of()
    nd, ns = nz * nx * ny * 2, ny * 2
    rows, width = block.shape
    cap, size = select.shape[1], w_out.shape[0]
    bf = jnp.bfloat16
    n = n_sems(nz, nx, ny)
    made = nd * cap
    gb = nx * ns if nx * ns <= 8 else ns
    tile = gb * cap
    sds = jax.ShapeDtypeStruct
    results = pl.pallas_call(expert_kernel,
        out_shape=(sds((nd, rows, width), bf), sds((made, width), bf), sds((made, width), bf), sds((made, size), bf),
            sds((made, 2 * size), bf), sds((nd, rows, width), bf), sds((made, width), bf)),
        in_specs=[VM, VM, VM, VM, ANY, VM, VM], out_specs=(ANY,) * 7,
        scratch_shapes=[pltpu.VMEM((gb, rows, width), bf), pltpu.VMEM((2, gb, rows, width), bf),
            pltpu.VMEM((tile, width), bf), pltpu.VMEM((tile, width), bf), pltpu.VMEM((tile, size), bf),
            pltpu.VMEM((tile, 2 * size), bf), pltpu.VMEM((gb, rows, width), bf), pltpu.VMEM((tile, width), bf),
            pltpu.SemaphoreType.DMA, pltpu.SemaphoreType.DMA, pltpu.SemaphoreType.DMA((2,)),
            pltpu.SemaphoreType.DMA((3, 2)), pltpu.SemaphoreType.DMA((n,)), pltpu.SemaphoreType.DMA((n,))],
        compiler_params=pltpu.CompilerParams(collective_id=cid, has_side_effects=True, vmem_limit_bytes=61 << 20),
        name="expert_pass")(block, select, select.transpose(0, 2, 1), jnp.broadcast_to(gate[:, :, None], gate.shape + (128,)),
            grads_all, w_in, w_out)
    return results[1:]


def expert_reduce_kernel(b_ref, sel_ref, selt_ref, gate_ref, g_ref, win_ref, wout_ref,
                         all_ref, in_ref, gr_ref, hid_ref, pg_ref, out_ref, sum_ref,
                         xt, gt, in_t, gr_t, hid_t, pg_t, out_t, back_t, give, acc, rc, ra1, rb1, ra2, rb2, rz,
                         local_sem, x_sem, g_sem, store_sem, out_sem, send, recv):
    p = Place()
    nz, nx, ny = p.nz, p.nx, p.ny
    ns = 2 * ny
    half = b_ref.shape[0] // 2
    cap = sel_ref.shape[1]
    size, width = wout_ref.shape
    f32, bf = jnp.float32, jnp.bfloat16
    A, B = pl.ds(0, half), pl.ds(half, half)
    F = pl.ds(0, 2 * half)
    p.greet(p.line_peers())
    own = pltpu.make_async_copy(b_ref, all_ref.at[p.index()], local_sem)
    own.start()
    s, r = Pool(send), Pool(recv)
    sent = []
    neg = lambda d, n: (n - d) % n

    def push(src_at, rows, to, first=False):
        i = p.index(*src_at)
        src = b_ref.at[rows] if first else all_ref.at[i, rows]
        cp = pltpu.make_async_remote_copy(src_ref=src, dst_ref=all_ref.at[i, rows], send_sem=s.take(),
            recv_sem=r.take(), device_id=p.dev(*to), device_id_type=MESH)
        cp.start()
        sent.append(cp)
        return cp

    first = {d: push((0, 0, 0, 0), F, (d, 0, 0, 0), True) for d in range(1, nz)}
    second_a, second_b, third, other = {}, {}, {}, {}

    def cross(at, rows, is_first=False):
        dx = neg(at[1], nx)
        other.setdefault((neg(at[0], nz), dx), []).append(push(at, rows, (0, 0, 0, 1), is_first))

    def stage_one(k):
        if k:
            first[k].wait_recv()
        at = (neg(k, nz), 0, 0, 0)
        for d in range(1, nx):
            second_a[k, d] = push(at, A, (0, d, 0, 0), k == 0)
        for d in range(1, ny):
            second_b[k, d] = push(at, B, (0, 0, d, 0), k == 0)
        for d in range(1, ny):
            third["a", k, 0, d] = push(at, A, (0, 0, d, 0), k == 0)
        for d in range(1, nx):
            third["b", k, 0, d] = push(at, B, (0, d, 0, 0), k == 0)
        cross(at, F, k == 0)

    def stage_two(k):
        for dx in range(1, nx):
            second_a[k, dx].wait_recv()
            at = (neg(k, nz), neg(dx, nx), 0, 0)
            for d in range(1, ny):
                third["a", k, dx, d] = push(at, A, (0, 0, d, 0))
            cross(at, A)
        for dy in range(1, ny):
            second_b[k, dy].wait_recv()
            at = (neg(k, nz), 0, neg(dy, ny), 0)
            for d in range(1, nx):
                third["b", k, dy, d] = push(at, B, (0, d, 0, 0))
            cross(at, B)

    def stage_three(k):
        for dx in range(nx):
            for d in range(1, ny):
                third["a", k, dx, d].wait_recv()
                cross((neg(k, nz), neg(dx, nx), neg(d, ny), 0), A)
        for dy in range(ny):
            for d in range(1, nx):
                third["b", k, dy, d].wait_recv()
                cross((neg(k, nz), neg(d, nx), neg(dy, ny), 0), B)

    gb = nx * ns

    def base_of(i):
        return p.at(neg(i, nz), 0, 0, 0)[0] * gb

    def load_x(i):
        return pltpu.make_async_copy(all_ref.at[pl.ds(base_of(i), gb)], xt, x_sem)

    def load_g(i):
        return pltpu.make_async_copy(g_ref.at[pl.ds(base_of(i), gb)], gt, g_sem)

    def stores(i, part):
        rows = pl.ds(base_of(i) * cap, gb * cap)
        pairs = [[(in_t, in_ref.at[rows]), (gr_t, gr_ref.at[rows])], [(hid_t, hid_ref.at[rows]), (pg_t, pg_ref.at[rows])]][part]
        return [pltpu.make_async_copy(a, b, store_sem.at[part, j]) for j, (a, b) in enumerate(pairs)]

    def compute(i):
        load_x(i).start()
        load_g(i).wait()
        base = base_of(i)
        if i:
            for cp in stores(i - 1, 0):
                cp.wait()
        load_x(i).wait()

        def pick(b, carry):
            rows = pl.ds(pl.multiple_of(b * cap, cap), cap)
            sel = sel_ref[base + b]
            in_t[rows, :] = jnp.dot(sel, xt[b], preferred_element_type=f32).astype(bf)
            gr_t[rows, :] = (jnp.dot(sel, gt[b], preferred_element_type=f32) * gate_ref[base + b][:, :1]).astype(bf)
            return carry

        lax.fori_loop(0, gb, pick, 0)
        if i + 1 < nz:
            load_g(i + 1).start()
        for cp in stores(i, 0):
            cp.start()
        if i:
            for cp in stores(i - 1, 1):
                cp.wait()
        wide = min(size, 256)

        def middle(j, carry):
            left = pl.ds(pl.multiple_of(j * wide, wide), wide)
            right = pl.ds(pl.multiple_of(size + j * wide, wide), wide)
            rows_in, rows_grad = in_t[...], gr_t[...]
            a = jnp.dot(rows_in, win_ref[:, left], preferred_element_type=f32)
            b = jnp.dot(rows_in, win_ref[:, right], preferred_element_type=f32)
            h = lax.dot_general(rows_grad, wout_ref[left, :], (((1,), (1,)), ((), ())), preferred_element_type=f32)
            sigma = 1.0 / (1.0 + jnp.exp(-a))
            active = a * sigma
            hid_t[:, left] = (active * b).astype(bf)
            pg_t[:, left] = (h * b * (sigma * (1.0 + a * (1.0 - sigma)))).astype(bf)
            pg_t[:, right] = (h * active).astype(bf)
            return carry

        lax.fori_loop(0, size // wide, middle, 0)
        for cp in stores(i, 1):
            cp.start()
        gates = jnp.concatenate([gate_ref[base + b][:, :1] for b in range(gb)], axis=0)

        def out_copy(j):
            t = lax.rem(j, 2)
            cols = pl.ds(pl.multiple_of(j * 256, 256), 256)
            return pltpu.make_async_copy(out_t.at[t], out_ref.at[pl.ds(base, gb), :, cols], out_sem.at[t])

        def final(j, carry):
            cols = pl.ds(pl.multiple_of(j * 256, 256), 256)
            out = jnp.dot(hid_t[...], wout_ref[:, cols], preferred_element_type=f32).astype(bf)
            weighted = (out.astype(f32) * gates).astype(bf)
            back_t[:, cols] = lax.dot_general(pg_t[...], win_ref[cols, :], (((1,), (1,)), ((), ())),
                preferred_element_type=f32).astype(bf)

            @pl.when(j >= 2)
            def _():
                out_copy(j - 2).wait()

            for b in range(gb):
                out_t[lax.rem(j, 2), b] = jnp.dot(selt_ref[base + b], weighted[b * cap:(b + 1) * cap],
                    preferred_element_type=f32).astype(bf)
            out_copy(j).start()
            return carry

        steps = width // 256
        lax.fori_loop(0, steps, final, 0)
        for j in range(max(0, steps - 2), steps):
            out_copy(j).wait()

    plane = [(dx, dy) for dx in reversed(range(nx)) for dy in reversed(range(ny))]
    slot = lambda dz, dx, dy: (dz * nx + dx) * ny + dy
    cores, ca, cb, za, zb, zz = {}, {}, {}, {}, {}, {}
    done = []

    def push_to(src, dst, to):
        cp = pltpu.make_async_remote_copy(src_ref=src, dst_ref=dst, send_sem=s.take(), recv_sem=r.take(),
            device_id=p.dev(*to), device_id_type=MESH)
        cp.start()
        sent.append(cp)
        return cp

    def term(i, index):
        b = index - base_of(i)
        rows = pl.ds(pl.multiple_of(b * cap, cap), cap)
        return jnp.dot(selt_ref[index], back_t[rows, :], preferred_element_type=f32)

    def add(dst, rows_, src):
        acc[dst, rows_, :] = (acc[dst, rows_, :].astype(f32) + src[...].astype(f32)).astype(acc.dtype)

    def sum_one(i):
        dz = neg(i, nz)
        for j, (dx, dy) in enumerate(plane):
            g = (i % 2) * len(plane) + j
            if i >= 2:
                old = cores[neg(i - 2, nz), dx, dy]
                old.wait_send()
                done.append(old)
            give[g] = term(i, p.index(dz, dx, dy, 1)).astype(bf)
            cores[dz, dx, dy] = push_to(give.at[g], rc.at[slot(dz, dx, dy)], (0, 0, 0, 1))
        for dx, dy in plane:
            t = slot(dz, dx, dy)
            mine = term(i, p.index(dz, dx, dy))
            cores[dz, dx, dy].wait_recv()
            acc[t] = (mine + rc[t].astype(f32)).astype(bf)
            if dy:
                ca[dz, dx, dy] = push_to(acc.at[t, A], ra1.at[dy - 1, dz * nx + dx], (0, 0, dy, 0))
            if dx:
                cb[dz, dx, dy] = push_to(acc.at[t, B], rb1.at[dx - 1, dz * ny + dy], (0, dx, 0, 0))

    def sum_two(i):
        dz = neg(i, nz)
        for dx in reversed(range(nx)):
            for dy in range(1, ny):
                ca[dz, dx, dy].wait_recv()
                add(slot(dz, dx, 0), A, ra1.at[dy - 1, dz * nx + dx])
            if dx:
                za[dz, dx] = push_to(acc.at[slot(dz, dx, 0), A], ra2.at[dx - 1, dz], (0, dx, 0, 0))
        for dy in reversed(range(ny)):
            for dx in range(1, nx):
                cb[dz, dx, dy].wait_recv()
                add(slot(dz, 0, dy), B, rb1.at[dx - 1, dz * ny + dy])
            if dy:
                zb[dz, dy] = push_to(acc.at[slot(dz, 0, dy), B], rb2.at[dy - 1, dz], (0, 0, dy, 0))

    def sum_three(i):
        dz = neg(i, nz)
        for dx in range(1, nx):
            za[dz, dx].wait_recv()
            add(slot(dz, 0, 0), A, ra2.at[dx - 1, dz])
        for dy in range(1, ny):
            zb[dz, dy].wait_recv()
            add(slot(dz, 0, 0), B, rb2.at[dy - 1, dz])
        if dz:
            zz[dz] = push_to(acc.at[slot(dz, 0, 0)], rz.at[dz - 1], (dz, 0, 0, 0))

    load_g(0).start()
    for k in range(nz + 2):
        if k < nz:
            stage_one(k)
        if 0 <= k - 1 < nz:
            stage_two(k - 1)
        if 0 <= k - 2 < nz:
            stage_three(k - 2)
            if k == 2:
                own.wait()
            for dx in range(nx):
                for cp in other[k - 2, dx]:
                    cp.wait_recv()
            compute(k - 2)
            sum_one(k - 2)
            if k - 3 >= 0:
                sum_two(k - 3)
            if k - 4 >= 0:
                sum_three(k - 4)
    sum_two(nz - 1)
    for i in range(max(0, nz - 2), nz):
        sum_three(i)
    total = acc[slot(0, 0, 0)].astype(f32)
    for dz in range(1, nz):
        zz[dz].wait_recv()
        total = total + rz[dz - 1].astype(f32)
    sum_ref[...] = total
    for part in range(2):
        for cp in stores(nz - 1, part):
            cp.wait()
    for cp in sent:
        if not any(cp is other_cp for other_cp in done):
            cp.wait_send()


def expert_reduce(block, select, gate, grads_all, w_in, w_out, cid):
    nz, nx, ny = grid_of()
    nd, gb = nz * nx * ny * 2, nx * ny * 2
    rows, width = block.shape
    half = rows // 2
    cap, size = select.shape[1], w_out.shape[0]
    bf = jnp.bfloat16
    n = n_sems(nz, nx, ny) + 2 * nz * nx * ny + nz * (nx + ny) + 2 * nz * (nx * (ny - 1) + ny * (nx - 1))
    made, tile, slots = nd * cap, gb * cap, nz * nx * ny
    sds = jax.ShapeDtypeStruct
    results = pl.pallas_call(expert_reduce_kernel,
        out_shape=(sds((nd, rows, width), bf), sds((made, width), bf), sds((made, width), bf), sds((made, size), bf),
            sds((made, 2 * size), bf), sds((nd, rows, width), bf), sds((rows, width), jnp.float32)),
        in_specs=[VM, VM, VM, VM, ANY, VM, VM], out_specs=(ANY,) * 6 + (VM,),
        scratch_shapes=[pltpu.VMEM((gb, rows, width), bf), pltpu.VMEM((gb, rows, width), bf),
            pltpu.VMEM((tile, width), bf), pltpu.VMEM((tile, width), bf), pltpu.VMEM((tile, size), bf),
            pltpu.VMEM((tile, 2 * size), bf), pltpu.VMEM((2, gb, rows, 256), bf), pltpu.VMEM((tile, width), bf),
            pltpu.VMEM((2 * nx * ny, rows, width), bf), pltpu.VMEM((slots, rows, width), bf), pltpu.VMEM((slots, rows, width), bf),
            pltpu.VMEM((ny - 1, nz * nx, half, width), bf), pltpu.VMEM((nx - 1, nz * ny, half, width), bf),
            pltpu.VMEM((nx - 1, nz, half, width), bf), pltpu.VMEM((ny - 1, nz, half, width), bf),
            pltpu.VMEM((nz - 1, rows, width), bf),
            pltpu.SemaphoreType.DMA, pltpu.SemaphoreType.DMA, pltpu.SemaphoreType.DMA,
            pltpu.SemaphoreType.DMA((2, 2)), pltpu.SemaphoreType.DMA((2,)),
            pltpu.SemaphoreType.DMA((n,)), pltpu.SemaphoreType.DMA((n,))],
        compiler_params=pltpu.CompilerParams(collective_id=cid, has_side_effects=True, vmem_limit_bytes=67043328),
        name="expert_reduce")(block, select, select.transpose(0, 2, 1), jnp.broadcast_to(gate[:, :, None], gate.shape + (128,)),
            grads_all, w_in, w_out)
    return results[1:]


def shard_peers(ny):
    return [(0, 0, dy, dc) for dy in range(ny) for dc in range(2) if dy or dc]


def weights_kernel(w_ref, wo_ref, t_ref, wall_ref, woall_ref, tall_ref, local_sem, send, recv):
    p = Place()
    nz, nx, ny = p.nz, p.nx, p.ny
    ns = ny * 2
    e, sh = lax.axis_index("expert"), lax.axis_index("shard")
    ne = nz * nx
    me = e * ns + sh
    to_e, to_s = me % ne, me // ne
    from_e, from_s = (sh * ne + e) // ns, (sh * ne + e) % ns
    moved = jnp.logical_not(jnp.logical_and(to_e == e, to_s == sh))
    peers = [q for q in p.line_peers() if not (q[2] or q[3])] + shard_peers(ny)
    barrier = pltpu.get_barrier_semaphore()
    for q in peers:
        pl.semaphore_signal(barrier, inc=1, device_id=p.dev(*q), device_id_type=MESH)

    @pl.when(moved)
    def _():
        pl.semaphore_signal(barrier, inc=1, device_id=(from_e, from_s), device_id_type=MESH)

    pl.semaphore_wait(barrier, len(peers) + moved.astype(jnp.int32))
    s, r = Pool(send), Pool(recv)
    sent = []
    neg = lambda d, n: (n - d) % n

    def push(src, dst, to):
        cp = pltpu.make_async_remote_copy(src_ref=src, dst_ref=dst, send_sem=s.take(), recv_sem=r.take(),
            device_id=p.dev(*to), device_id_type=MESH)
        cp.start()
        sent.append(cp)
        return cp

    mixed = []
    for q in shard_peers(ny):
        _, _, y, c = p.at(*q)
        mixed.append(push(w_ref.at[y * 2 + c], wall_ref.at[me], q))
    own_w = pltpu.make_async_copy(w_ref.at[sh], wall_ref.at[me], local_sem.at[0])
    own_w.start()
    entry_send, entry_recv = s.take(), r.take()
    entry = pltpu.make_async_remote_copy(src_ref=wo_ref, dst_ref=woall_ref.at[to_e], send_sem=entry_send,
        recv_sem=entry_recv, device_id=(to_e, to_s), device_id_type=MESH)
    stay = pltpu.make_async_copy(wo_ref, woall_ref.at[e], local_sem.at[1])

    @pl.when(moved)
    def _():
        entry.start()

    @pl.when(jnp.logical_not(moved))
    def _():
        stay.start()

    own_t = pltpu.make_async_copy(t_ref, tall_ref.at[sh], local_sem.at[2])
    own_t.start()
    toks = {}
    for d in range(1, ny):
        toks[d] = push(t_ref, tall_ref.at[sh], (0, 0, d, 0))
    tail = [push(t_ref, tall_ref.at[sh], (0, 0, 0, 1))]

    def block(ref, zz, size):
        z, x, _, _ = p.at(zz, 0, 0, 0)
        return ref.at[pl.ds((z * nx + x) * size, size)]

    def spread_first(ref, size):
        lines = {}
        for d in range(1, nz):
            b = block(ref, 0, size)
            lines[d] = push(b, b, (d, 0, 0, 0))
        for d in range(1, nx):
            b = block(ref, 0, size)
            tail.append(push(b, b, (0, d, 0, 0)))
        return lines

    def spread_next(ref, size, lines, d):
        lines[d].wait_recv()
        for dx in range(1, nx):
            b = block(ref, neg(d, nz), size)
            tail.append(push(b, b, (0, dx, 0, 0)))

    own_w.wait()
    for cp in mixed:
        cp.wait_recv()
    lines_w = spread_first(wall_ref, ns)

    @pl.when(moved)
    def _():
        entry.wait()

    @pl.when(jnp.logical_not(moved))
    def _():
        stay.wait()

    lines_o = spread_first(woall_ref, 1)
    for d in range(1, ny):
        toks[d].wait_recv()
        _, _, y, c = p.at(0, 0, neg(d, ny), 0)
        b = tall_ref.at[y * 2 + c]
        tail.append(push(b, b, (0, 0, 0, 1)))
    for d in range(1, nz):
        spread_next(wall_ref, ns, lines_w, d)
    for d in range(1, nz):
        spread_next(woall_ref, 1, lines_o, d)
    for cp in tail:
        cp.wait_recv()
    for cp in sent:
        cp.wait_send()
    own_t.wait()


def gather_weights(w, wo, t, cid):
    nz, nx, ny = grid_of()
    ns, ne = ny * 2, nz * nx
    n = 2 * ns + 2 + 2 * (nz + nx + nz * nx) + 2 * ny + 8
    return pl.pallas_call(weights_kernel,
        out_shape=(jax.ShapeDtypeStruct((ne * ns,) + w.shape[1:], w.dtype),
            jax.ShapeDtypeStruct((ne,) + wo.shape, wo.dtype), jax.ShapeDtypeStruct((ns,) + t.shape, t.dtype)),
        in_specs=[VM, VM, VM], out_specs=(ANY, ANY, ANY),
        scratch_shapes=[pltpu.SemaphoreType.DMA((3,)), pltpu.SemaphoreType.DMA((n,)), pltpu.SemaphoreType.DMA((n,))],
        compiler_params=pltpu.CompilerParams(collective_id=cid, has_side_effects=True),
        name="gather_weights")(w, wo, t)


def pack_gather_kernel(t_ref, o_ref, local_sem, send, recv):
    p = Place()
    ny = p.ny
    p.greet([(0, 0, d, 0) for d in range(1, ny)] + [(0, 0, 0, 1)])
    sh = lax.axis_index("shard")
    own = pltpu.make_async_copy(t_ref, o_ref.at[sh], local_sem)
    own.start()
    s, r = Pool(send), Pool(recv)
    sent, tail, along = [], [], {}
    rows = t_ref.shape[0]
    pieces = 4

    def push(src, dst, to):
        cp = pltpu.make_async_remote_copy(src_ref=src, dst_ref=dst, send_sem=s.take(), recv_sem=r.take(),
            device_id=p.dev(*to), device_id_type=MESH)
        cp.start()
        sent.append(cp)
        return cp

    part = [pl.ds(k * (rows // pieces), rows // pieces) for k in range(pieces)]
    for k in range(pieces):
        for d in range(1, ny):
            along[k, d] = push(t_ref.at[part[k]], o_ref.at[sh, part[k]], (0, 0, d, 0))
    tail.append(push(t_ref, o_ref.at[sh], (0, 0, 0, 1)))
    for k in range(pieces):
        for d in range(1, ny):
            along[k, d].wait_recv()
            _, _, y, c = p.at(0, 0, (ny - d) % ny, 0)
            b = o_ref.at[y * 2 + c, part[k]]
            tail.append(push(b, b, (0, 0, 0, 1)))
    for cp in tail:
        cp.wait_recv()
    for cp in sent:
        cp.wait_send()
    own.wait()


def pack_gather(t, cid):
    nz, nx, ny = grid_of()
    n = 8 * ny
    return pl.pallas_call(pack_gather_kernel,
        out_shape=jax.ShapeDtypeStruct((ny * 2,) + t.shape, t.dtype), in_specs=[VM], out_specs=VM,
        scratch_shapes=[pltpu.SemaphoreType.DMA, pltpu.SemaphoreType.DMA((n,)), pltpu.SemaphoreType.DMA((n,))],
        compiler_params=pltpu.CompilerParams(collective_id=cid, has_side_effects=True),
        name="pack_gather")(t)


def pack_reduce_body(p, g_ref, out_ref, acc, rc, ry, push, pieces=4):
    ny = p.ny
    rows = g_ref.shape[1]
    step = rows // pieces
    part = [pl.ds(k * step, step) for k in range(pieces)]
    order = list(range(1, ny)) + [0]
    cores, along = {}, {}
    for k in range(pieces):
        for dy in order:
            _, _, y, c = p.at(0, 0, dy, 1)
            cores[k, dy] = push(g_ref.at[y * 2 + c, part[k]], rc.at[dy, part[k]], (0, 0, 0, 1))

    def first():
        for k in range(pieces):
            for dy in order:
                _, _, y, c = p.at(0, 0, dy, 0)
                cores[k, dy].wait_recv()
                both = g_ref[y * 2 + c, part[k], :].astype(jnp.float32) + rc[dy, part[k], :].astype(jnp.float32)
                if dy:
                    acc[dy - 1, part[k], :] = both.astype(acc.dtype)
                    along[k, dy] = push(acc.at[dy - 1, part[k]], ry.at[dy - 1, part[k]], (0, 0, dy, 0))
                else:
                    out_ref[part[k], :] = both

    def second():
        for k in range(pieces):
            for dy in range(1, ny):
                along[k, dy].wait_recv()
                out_ref[part[k], :] = out_ref[part[k], :] + ry[dy - 1, part[k], :].astype(jnp.float32)

    return first, second


def pack_reduce_kernel(g_ref, out_ref, acc, rc, ry, send, recv):
    p = Place()
    p.greet([(0, 0, d, 0) for d in range(1, p.ny)] + [(0, 0, 0, 1)])
    s, r = Pool(send), Pool(recv)
    sent = []

    def push(src, dst, to):
        cp = pltpu.make_async_remote_copy(src_ref=src, dst_ref=dst, send_sem=s.take(), recv_sem=r.take(),
            device_id=p.dev(*to), device_id_type=MESH)
        cp.start()
        sent.append(cp)
        return cp

    first, second = pack_reduce_body(p, g_ref, out_ref, acc, rc, ry, push)
    first()
    second()
    for cp in sent:
        cp.wait_send()


def pack_scratch(ny, rows, width, dt):
    return [pltpu.VMEM((ny - 1, rows, width), dt), pltpu.VMEM((ny, rows, width), dt), pltpu.VMEM((ny - 1, rows, width), dt)]


def pack_reduce(terms, cid):
    nz, nx, ny = grid_of()
    ns, rows, width = terms.shape
    n = 8 * ny
    return pl.pallas_call(pack_reduce_kernel,
        out_shape=jax.ShapeDtypeStruct((rows, width), jnp.float32), in_specs=[VM], out_specs=VM,
        scratch_shapes=pack_scratch(ny, rows, width, terms.dtype)
            + [pltpu.SemaphoreType.DMA((n,)), pltpu.SemaphoreType.DMA((n,))],
        compiler_params=pltpu.CompilerParams(collective_id=cid, has_side_effects=True, vmem_limit_bytes=40 << 20),
        name="pack_reduce")(terms)


def grads_kernel(wo_ref, w_ref, s_ref, n_ref, wo_out, w_out, s_out, n_out,
                 wo_x, wo_z, wo_l, wo_r, w_x, w_z, w_l, w_r, s_x, s_z, s_l, acc, rc, ry, load_sem, send, recv):
    p = Place()
    nz, nx, ny = p.nz, p.nx, p.ny
    ns, ne = ny * 2, nz * nx
    e, sh = lax.axis_index("expert"), lax.axis_index("shard")
    me = e * ns + sh
    own_e, own_s = (sh * ne + e) // ns, (sh * ne + e) % ns
    from_e, from_s = me % ne, me // ne
    moved = jnp.logical_not(jnp.logical_and(own_e == e, own_s == sh))
    peers = [q for q in p.line_peers() if not (q[2] or q[3])] + shard_peers(ny)
    barrier = pltpu.get_barrier_semaphore()
    for q in peers:
        pl.semaphore_signal(barrier, inc=1, device_id=p.dev(*q), device_id_type=MESH)

    @pl.when(moved)
    def _():
        pl.semaphore_signal(barrier, inc=1, device_id=(from_e, from_s), device_id_type=MESH)

    pl.semaphore_wait(barrier, len(peers) + moved.astype(jnp.int32))
    s, r = Pool(send), Pool(recv)
    sent = []

    def push(src, dst, to):
        cp = pltpu.make_async_remote_copy(src_ref=src, dst_ref=dst, send_sem=s.take(), recv_sem=r.take(),
            device_id=p.dev(*to), device_id_type=MESH)
        cp.start()
        sent.append(cp)
        return cp

    zs = list(range(1, nz)) + [0]
    jobs = [(w_ref, w_x, w_z, w_l, ns, 0), (s_ref, s_x, s_z, s_l, ns, nz), (wo_ref, wo_x, wo_z, wo_l, 1, 2 * nz)]

    def group(ref, dz, dx, size):
        z, x, _, _ = p.at(dz, dx, 0, 0)
        return ref.at[pl.ds((z * nx + x) * size, size)]

    xs, loads, lines = {}, {}, {}
    for j, (ref, x_buf, z_buf, l_buf, size, base) in enumerate(jobs):
        for dz in zs:
            for dx in range(1, nx):
                xs[j, dz, dx] = push(group(ref, dz, dx, size), x_buf.at[dx - 1, dz], (0, dx, 0, 0))
            loads[j, dz] = pltpu.make_async_copy(group(ref, dz, 0, size), l_buf.at[dz], load_sem.at[base + dz])
            loads[j, dz].start()
    first, second = pack_reduce_body(p, n_ref, n_out, acc, rc, ry, push)
    first()
    for j, (ref, x_buf, z_buf, l_buf, size, base) in enumerate(jobs):
        for dz in zs:
            loads[j, dz].wait()
            for dx in range(1, nx):
                xs[j, dz, dx].wait_recv()
            total = l_buf[dz].astype(jnp.float32)
            for dx in range(1, nx):
                total = total + x_buf[dx - 1, dz].astype(jnp.float32)
            l_buf[dz] = total.astype(l_buf.dtype)
            if dz:
                lines[j, dz] = push(l_buf.at[dz], z_buf.at[dz - 1], (dz, 0, 0, 0))
    second()
    last = []
    entry = pltpu.make_async_remote_copy(src_ref=wo_l.at[0, 0], dst_ref=wo_r, send_sem=s.take(),
        recv_sem=r.take(), device_id=(own_e, own_s), device_id_type=MESH)
    for j, (ref, x_buf, z_buf, l_buf, size, base) in enumerate(jobs):
        total = l_buf[0].astype(jnp.float32)
        for d in range(1, nz):
            lines[j, d].wait_recv()
            total = total + z_buf[d - 1].astype(jnp.float32)
        l_buf[0] = total.astype(l_buf.dtype)
        if j == 0:
            for q in shard_peers(ny):
                _, _, y, c = p.at(*q)
                last.append(push(l_buf.at[0, y * 2 + c], w_r.at[sh], q))
            w_r[sh] = l_buf[0, sh]
        elif j == 1:
            for q in shard_peers(ny):
                _, _, y, c = p.at(*q)
                last.append(push(l_buf.at[0, y * 2 + c], s_out.at[sh], q))
            s_out[sh] = l_buf[0, sh]

    @pl.when(moved)
    def _():
        entry.start()

    for cp in last:
        cp.wait_recv()
    w_out[...] = w_r[...].astype(jnp.float32)

    @pl.when(moved)
    def _():
        entry.wait()
        wo_out[...] = wo_r[...].astype(jnp.float32)

    @pl.when(jnp.logical_not(moved))
    def _():
        wo_out[...] = wo_l[0, 0].astype(jnp.float32)

    for cp in sent:
        cp.wait_send()


def reduce_grads(wo, w, small, inp, cid):
    nz, nx, ny = grid_of()
    ns, ne = ny * 2, nz * nx
    bf, f32 = jnp.bfloat16, jnp.float32
    rows_o, width = wo.shape[1:]
    rows_w, cb = w.shape[1:]
    rows_n = inp.shape[1]
    n = 3 * nz * nx + 3 * nz + 2 * ns + 8 * ny + 8
    small_block = small.shape[1:]
    return pl.pallas_call(grads_kernel,
        out_shape=(jax.ShapeDtypeStruct((rows_o, width), f32), jax.ShapeDtypeStruct((ns, rows_w, cb), f32),
            jax.ShapeDtypeStruct((ns,) + small_block, f32), jax.ShapeDtypeStruct((rows_n, width), f32)),
        in_specs=[ANY, ANY, ANY, VM], out_specs=(VM, VM, VM, VM),
        scratch_shapes=[pltpu.VMEM((nx - 1, nz, 1, rows_o, width), bf), pltpu.VMEM((nz - 1, 1, rows_o, width), bf),
            pltpu.VMEM((nz, 1, rows_o, width), bf), pltpu.VMEM((rows_o, width), bf),
            pltpu.VMEM((nx - 1, nz, ns, rows_w, cb), bf), pltpu.VMEM((nz - 1, ns, rows_w, cb), bf),
            pltpu.VMEM((nz, ns, rows_w, cb), bf), pltpu.VMEM((ns, rows_w, cb), bf),
            pltpu.VMEM((nx - 1, nz, ns) + small_block, f32), pltpu.VMEM((nz - 1, ns) + small_block, f32),
            pltpu.VMEM((nz, ns) + small_block, f32)]
            + pack_scratch(ny, rows_n, width, bf)
            + [pltpu.SemaphoreType.DMA((3 * nz,)), pltpu.SemaphoreType.DMA((n,)), pltpu.SemaphoreType.DMA((n,))],
        compiler_params=pltpu.CompilerParams(collective_id=cid, has_side_effects=True, vmem_limit_bytes=56 << 20),
        name="reduce_grads")(wo, w, small, inp)


QUERY_HEADS = 32
KEY_VALUE_HEADS = 4
HEAD = 128
EPSILON = 1e-06
THETA = 1000000.0


def normed(raw, gain):
    scale = lax.rsqrt(jnp.mean(raw * raw, axis=-1, keepdims=True) + EPSILON)
    hat = raw * scale
    return scale, hat, hat * gain


def turned(v, cosine, sine):
    return v * cosine + pltpu.roll(v, HEAD // 2, 1) * sine


def turned_back(g, cosine, sine):
    return g * cosine + pltpu.roll(g * sine, HEAD // 2, 1)


def weights_of(queries, keys, mask):
    scores = lax.dot_general(queries, keys, (((1,), (1,)), ((), ())), preferred_element_type=jnp.float32)
    scores = scores * HEAD ** (-0.5) + mask
    highest = jnp.max(scores, axis=-1, keepdims=True)
    powers = jnp.exp(scores - highest)
    return powers * (1.0 / jnp.sum(powers, axis=-1, keepdims=True))


def attend_kernel(q_ref, k_ref, v_ref, gq_ref, gk_ref, cos_ref, sin_ref, mask_ref, o_ref):
    bf = jnp.bfloat16
    cosine, sine = cos_ref[...], sin_ref[...]
    queries = turned(normed(q_ref[...], gq_ref[...])[2], cosine, sine).astype(bf)
    keys = turned(normed(k_ref[...], gk_ref[...])[2], cosine, sine).astype(bf)
    probs = weights_of(queries, keys, mask_ref[...]).astype(bf)
    o_ref[...] = jnp.dot(probs, v_ref[...].astype(bf), preferred_element_type=jnp.float32).astype(bf)


def attend_back_kernel(per, q_ref, k_ref, v_ref, gq_ref, gk_ref, cos_ref, sin_ref, mask_ref, o_ref, do_ref, inv_ref,
                       dq_ref, dk_ref, dv_ref, dgq_ref, dgk_ref, dk_acc, dv_acc):
    bf, f32 = jnp.bfloat16, jnp.float32
    h = pl.program_id(0)
    cosine, sine = cos_ref[...], sin_ref[...]
    gain_q, gain_k = gq_ref[...], gk_ref[...]
    q_scale, q_hat, q_gained = normed(q_ref[...], gain_q)
    k_scale, k_hat, k_gained = normed(k_ref[...], gain_k)
    queries = turned(q_gained, cosine, sine).astype(bf)
    keys = turned(k_gained, cosine, sine).astype(bf)
    probs = weights_of(queries, keys, mask_ref[...])
    out_grad = do_ref[...]
    delta = jnp.sum(out_grad.astype(f32) * o_ref[...].astype(f32), axis=-1, keepdims=True)
    prob_grad = lax.dot_general(out_grad, v_ref[...].astype(bf), (((1,), (1,)), ((), ())), preferred_element_type=f32)
    score_grad = (probs * (prob_grad - delta)).astype(bf)
    factor = HEAD ** (-0.5)
    over_rows = (((0,), (0,)), ((), ()))
    dk_here = lax.dot_general(score_grad, queries, over_rows, preferred_element_type=f32)
    dv_here = lax.dot_general(probs.astype(bf), out_grad, over_rows, preferred_element_type=f32)

    @pl.when(h % per == 0)
    def _():
        dk_acc[...] = dk_here
        dv_acc[...] = dv_here

    @pl.when(h % per != 0)
    def _():
        dk_acc[...] += dk_here
        dv_acc[...] += dv_here

    @pl.when(h == 0)
    def _():
        dgq_ref[...] = jnp.zeros_like(dgq_ref)
        dgk_ref[...] = jnp.zeros_like(dgk_ref)

    def raw_grad(grad, scale, hat, gain, gain_grad_ref):
        gained = turned_back(grad, cosine, sine)
        gain_grad_ref[0:1, :] += jnp.sum(gained * hat, axis=0, keepdims=True)
        inner = gained * gain
        return scale * (inner - hat * jnp.mean(inner * hat, axis=-1, keepdims=True))

    query_grad = jnp.dot(score_grad, keys, preferred_element_type=f32) * factor
    dq_ref[...] = (raw_grad(query_grad, q_scale, q_hat, gain_q, dgq_ref) * inv_ref[...]).astype(bf)

    @pl.when(h % per == per - 1)
    def _():
        dk_ref[...] = (raw_grad(dk_acc[...] * factor, k_scale, k_hat, gain_k, dgk_ref) * inv_ref[...]).astype(bf)
        dv_ref[...] = (dv_acc[...] * inv_ref[...]).astype(bf)


def head_specs(length, heads, kv_heads, per):
    block = (length, HEAD)
    same = lambda h: (0, 0)
    return block, [pl.BlockSpec(block, lambda h: (0, h)), pl.BlockSpec(block, lambda h: (0, heads + h // per)),
        pl.BlockSpec(block, lambda h: (0, heads + kv_heads + h // per)), pl.BlockSpec((1, HEAD), same),
        pl.BlockSpec((1, HEAD), same), pl.BlockSpec(block, same), pl.BlockSpec(block, same),
        pl.BlockSpec((length, length), same)]


def attend(projected, shared, heads, kv_heads):
    length = projected.shape[0]
    block, specs = head_specs(length, heads, kv_heads, heads // kv_heads)
    return pl.pallas_call(attend_kernel, grid=(heads,),
        out_shape=jax.ShapeDtypeStruct((length, heads * HEAD), jnp.bfloat16),
        in_specs=specs, out_specs=pl.BlockSpec(block, lambda h: (0, h)),
        compiler_params=pltpu.CompilerParams(vmem_limit_bytes=56 << 20),
        name="attend")(projected, projected, projected, *shared)


def attend_back(projected, shared, attn, attn_grad, inverse, heads, kv_heads):
    length = projected.shape[0]
    per = heads // kv_heads
    block, specs = head_specs(length, heads, kv_heads, per)
    at_head = pl.BlockSpec(block, lambda h: (0, h))
    at_group = pl.BlockSpec(block, lambda h: (0, h // per))
    small = pl.BlockSpec((8, HEAD), lambda h: (0, 0))
    sds, bf, f32 = jax.ShapeDtypeStruct, jnp.bfloat16, jnp.float32
    return pl.pallas_call(functools.partial(attend_back_kernel, per), grid=(heads,),
        out_shape=(sds((length, heads * HEAD), bf), sds((length, kv_heads * HEAD), bf), sds((length, kv_heads * HEAD), bf),
            sds((8, HEAD), f32), sds((8, HEAD), f32)),
        in_specs=specs + [at_head, at_head, pl.BlockSpec((length, 1), lambda h: (0, 0))],
        out_specs=(at_head, at_group, at_group, small, small),
        scratch_shapes=[pltpu.VMEM(block, f32), pltpu.VMEM(block, f32)],
        compiler_params=pltpu.CompilerParams(vmem_limit_bytes=58 << 20),
        name="attend_back")(projected, projected, projected, *shared, attn, attn_grad, inverse)


def segment_starts(segment):
    index = jnp.arange(segment.shape[0], dtype=jnp.int32)
    same = segment[:, None] == segment[None, :]
    return jnp.min(jnp.where(same, index[None, :], segment.shape[0]), axis=1)


def shards(tokens_in, out_grad, segment_ids, expert_ids, route_weights, attn_gain, qkv_weight, q_gain, k_gain,
           out_weight, moe_gain, expert_in, expert_out):
    f32, bf = jnp.float32, jnp.bfloat16
    n_expert, n_shard = lax.axis_size("expert"), lax.axis_size("shard")
    nd = n_expert * n_shard
    rows, width = tokens_in.shape
    me = lax.axis_index("expert") * n_shard + lax.axis_index("shard")
    heads = QUERY_HEADS // n_shard
    kv_heads = max(1, KEY_VALUE_HEADS // n_shard)
    copies = max(1, n_shard // KEY_VALUE_HEADS)
    q_cols, kv_cols = heads * HEAD, kv_heads * HEAD
    q_all, kv_all = QUERY_HEADS * HEAD, KEY_VALUE_HEADS * HEAD
    wide = qkv_weight.shape[0]

    scaled = (qkv_weight.astype(f32) * attn_gain.astype(f32)[:, None]).astype(bf)

    def by_shard(part, cols, count):
        part = part.reshape(wide, n_shard // count, 1, cols)
        return jnp.broadcast_to(part, (wide, n_shard // count, count, cols)).reshape(wide, n_shard, cols)

    pieces = jnp.concatenate([by_shard(scaled[:, :q_all], q_cols, 1),
        by_shard(scaled[:, q_all:q_all + kv_all], kv_cols, copies),
        by_shard(scaled[:, q_all + kv_all:], kv_cols, copies)], axis=2).transpose(1, 0, 2)
    weights, out_rows, pack = gather_weights(pieces, out_weight, tokens_in, 0)
    weights = weights.reshape(width, -1)
    out_rows = out_rows.reshape(heads * HEAD, width)
    pack = pack.reshape(n_shard * rows, width)
    length = pack.shape[0]

    high = route_weights.astype(bf)
    rest = route_weights - high.astype(f32)
    middle = rest.astype(bf)
    low = (rest - middle.astype(f32)).astype(bf)
    top = expert_ids.shape[1]
    gains = jnp.zeros((rows,), bf)
    at = 0
    for g in (moe_gain, q_gain, k_gain):
        gains = lax.dynamic_update_slice(gains, g, (at,))
        at += g.shape[0]
    extra = jnp.concatenate([expert_ids.astype(bf), high, middle, low, gains[:, None]], axis=1)
    extra = jnp.pad(extra, ((0, 0), (0, 128 - extra.shape[1])))
    both = ("expert", "shard")
    info = lax.all_gather(extra, both, axis=0, tiled=False).astype(f32)
    grads_all = lax.all_gather(out_grad, both, axis=0, tiled=True).reshape(nd, rows, width)
    ids_all = info[:, :, :top]
    weights_all = info[:, :, top:2 * top] + info[:, :, 2 * top:3 * top] + info[:, :, 3 * top:4 * top]
    gain_col = info[:, :, 4 * top]
    g0, g1, g2 = moe_gain.shape[0], q_gain.shape[0], k_gain.shape[0]
    moe_scale = gain_col[:, :g0].reshape(-1)
    query_gain = gain_col[:, g0:g0 + g1].reshape(-1)
    key_gain = gain_col[:, g0 + g1:g0 + g1 + g2].reshape(-1)

    pack_f32 = pack.astype(f32)
    inverse = lax.rsqrt(jnp.mean(pack_f32 * pack_f32, axis=-1, keepdims=True) + EPSILON)
    projected = jnp.dot(pack, weights, preferred_element_type=f32) * inverse
    segment = segment_ids[0]
    index = jnp.arange(length, dtype=jnp.int32)
    position = (index - segment_starts(segment)).astype(f32)
    freqs = jnp.exp(jnp.arange(HEAD // 2, dtype=f32) * (-2.0 * math.log(THETA) / HEAD))
    angles = position[:, None] * freqs[None, :]
    cosine, sine = jnp.cos(angles), jnp.sin(angles)
    allowed = (segment[:, None] == segment[None, :]) & (index[None, :] <= index[:, None])
    shared = (query_gain[None], key_gain[None], jnp.concatenate([cosine, cosine], axis=1),
        jnp.concatenate([-sine, sine], axis=1), jnp.where(allowed, 0.0, -1e30).astype(f32))
    attn_flat = attend(projected, shared, heads, kv_heads)
    mixed = jnp.dot(attn_flat, out_rows, preferred_element_type=f32).astype(bf)
    hidden_state = tokens_in.astype(f32) + pack_reduce(mixed.reshape(n_shard, rows, width), 2)
    hidden_inverse = lax.rsqrt(jnp.mean(hidden_state * hidden_state, axis=-1, keepdims=True) + EPSILON)
    hidden_norm = hidden_state * hidden_inverse
    moe_in = (hidden_norm * moe_scale).astype(bf)

    cap = max(2, 2 * rows * top // nd)
    hit = ids_all == me.astype(f32)
    any_hit = jnp.any(hit, axis=-1)
    gate = jnp.sum(jnp.where(hit, weights_all, 0.0), axis=-1)
    lower = (jnp.arange(rows)[:, None] <= jnp.arange(rows)[None, :]).astype(bf)
    rank = jnp.dot(any_hit.astype(bf), lower, preferred_element_type=f32) - 1.0
    chosen = (jnp.arange(cap, dtype=f32)[None, :, None] == rank[:, None, :]) & any_hit[:, None, :]
    slot_gate = jnp.sum(jnp.where(chosen, gate[:, None, :], 0.0), axis=-1)
    select = chosen.astype(bf)
    experts = (moe_in, select, slot_gate, grads_all, expert_in[0], expert_out[0])
    if 16 * nd * rows * width // 5 <= 28 << 20:
        in_rows, grad_rows, hidden, pre_grad, out_terms, moe_grad = expert_reduce(*experts, 3)
    else:
        in_rows, grad_rows, hidden, pre_grad, out_terms, rows_grad = expert_pass(*experts, 1)
        moe_grad = reduce_rows(rows_grad.reshape(nd, cap, width), select, 5)
    expert_in_grad = jnp.einsum("rd,rc->dc", in_rows, pre_grad, preferred_element_type=f32)[None]
    expert_out_grad = jnp.einsum("rf,rd->fd", hidden, grad_rows, preferred_element_type=f32)[None]

    scaled_grad = moe_grad * moe_scale
    moe_gain_grad = jnp.sum(moe_grad * hidden_norm, axis=0)
    residual = out_grad.astype(f32) + hidden_inverse * (
        scaled_grad - hidden_norm * jnp.mean(scaled_grad * hidden_norm, axis=-1, keepdims=True))
    residual_pack = pack_gather(residual.astype(bf), 6).reshape(length, width)
    out_terms, residual_pack = lax.optimization_barrier((out_terms, residual_pack))
    moe_sum = lax.psum_scatter(out_terms.reshape(nd * rows, width), both, scatter_dimension=0, tiled=True).astype(f32)
    block_output = (hidden_state + moe_sum).astype(bf)
    out_term = jnp.einsum("tc,td->cd", attn_flat, residual_pack, preferred_element_type=f32).astype(bf)
    attn_grad = jnp.einsum("td,cd->tc", residual_pack, out_rows, preferred_element_type=f32).astype(bf)
    query_part, key_part, value_part, query_gain_grad, key_gain_grad = attend_back(projected, shared, attn_flat, attn_grad,
        inverse, heads, kv_heads)
    query_gain_grad, key_gain_grad = query_gain_grad[0], key_gain_grad[0]
    projected_grad = jnp.concatenate([query_part, key_part, value_part], axis=1)
    qkv_term = jnp.einsum("td,tc->dc", pack, projected_grad, preferred_element_type=f32).astype(bf)
    input_term = jnp.einsum("tc,dc->td", projected_grad, weights, preferred_element_type=f32).astype(bf)

    def lanes(v):
        v = v.reshape(nd, -1)
        return jnp.pad(v, ((0, 0), (0, 128 - v.shape[1])))[:, None]

    expert_in_grad, expert_out_grad, input_term = lax.optimization_barrier((expert_in_grad, expert_out_grad, input_term))
    small = jnp.concatenate([lanes(moe_gain_grad), lanes(query_gain_grad), lanes(key_gain_grad),
        jnp.zeros((nd, 5, 128), f32)], axis=1)
    out_weight_grad, qkv_part, small_sum, input_sum = reduce_grads(out_term.reshape(n_expert, -1, width),
        qkv_term.reshape(nd, wide, -1), small, input_term.reshape(n_shard, rows, width), 7)
    small_sum = jnp.sum(small_sum, axis=0)

    def whole_cols(part, count):
        part = part.transpose(1, 0, 2).reshape(wide, n_shard // count, count, -1)
        return jnp.sum(part, axis=2).reshape(wide, -1)

    raw = jnp.concatenate([whole_cols(qkv_part[:, :, :q_cols], 1), whole_cols(qkv_part[:, :, q_cols:q_cols + kv_cols], copies),
        whole_cols(qkv_part[:, :, q_cols + kv_cols:], copies)], axis=1)
    attn_gain_grad = jnp.sum(raw * qkv_weight.astype(f32), axis=1)
    qkv_weight_grad = raw * attn_gain.astype(f32)[:, None]
    own = tokens_in.astype(f32)
    own_norm = own * lax.rsqrt(jnp.mean(own * own, axis=-1, keepdims=True) + EPSILON)
    input_grad = (residual + input_sum - own_norm * jnp.mean(input_sum * own_norm, axis=-1, keepdims=True)).astype(bf)
    return (block_output, input_grad, attn_gain_grad, qkv_weight_grad, small_sum[1, :g1], small_sum[2, :g2],
        out_weight_grad, small_sum[0, :g0], expert_in_grad, expert_out_grad)


def solution(mesh):
    both = ("expert", "shard")
    row, rows2, rows3 = P(both), P(both, None), P(both, None, None)
    return jax.shard_map(
        shards, mesh=mesh,
        in_specs=(rows2, rows2, P("expert", None), rows2, rows2, row, rows2, row, row, rows2, row, rows3, rows3),
        out_specs=(rows2, rows2, row, rows2, row, row, rows2, row, rows3, rows3),
        check_vma=False,
    )
```

```python
import functools
import math
import jax, jax.numpy as jnp
from jax import lax
from jax.experimental import pallas as pl
from jax.experimental.pallas import tpu as pltpu
from jax.sharding import PartitionSpec as P
MESH = pl.DeviceIdType.MESH
ANY = pl.BlockSpec(memory_space=pl.ANY)
VM = pl.BlockSpec(memory_space=pltpu.VMEM)

def grid_of():
    n_expert, n_shard = lax.axis_size("expert"), lax.axis_size("shard")
    ny = n_shard // 2
    nx = min(ny, n_expert)
    return n_expert // nx, nx, ny

class Place:
    def __init__(self):
        self.nz, self.nx, self.ny = grid_of()
        e, s = lax.axis_index("expert"), lax.axis_index("shard")
        self.z, self.x = e // self.nx, e % self.nx
        self.y, self.c = s // 2, s % 2
    def dev(self, dz=0, dx=0, dy=0, dc=0):
        z, x, y, c = self.at(dz, dx, dy, dc)
        return (z * self.nx + x, y * 2 + c)
    def at(self, dz=0, dx=0, dy=0, dc=0):
        z = lax.rem(self.z + dz + self.nz, self.nz) if dz else self.z
        x = lax.rem(self.x + dx + self.nx, self.nx) if dx else self.x
        y = lax.rem(self.y + dy + self.ny, self.ny) if dy else self.y
        c = 1 - self.c if dc else self.c
        return z, x, y, c
    def index(self, dz=0, dx=0, dy=0, dc=0):
        z, x, y, c = self.at(dz, dx, dy, dc)
        return ((z * self.nx + x) * self.ny + y) * 2 + c
    def greet(self, peers):
        barrier = pltpu.get_barrier_semaphore()
        for p in peers:
            pl.semaphore_signal(barrier, inc=1, device_id=self.dev(*p), device_id_type=MESH)
        pl.semaphore_wait(barrier, len(peers))
    def line_peers(self):
        return ([(d, 0, 0, 0) for d in range(1, self.nz)] + [(0, d, 0, 0) for d in range(1, self.nx)]
                + [(0, 0, d, 0) for d in range(1, self.ny)] + [(0, 0, 0, 1)])

class Pool:
    def __init__(self, sems):
        self.sems, self.used = sems, 0
    def take(self):
        self.used += 1
        return self.sems.at[self.used - 1]

def n_sems(nz, nx, ny):
    return (nz - 1) + nz * (nx - 1 + ny - 1 + 1) + nz * (nx * (ny - 1) + ny * (nx - 1)) + nz * (nx - 1 + ny - 1) + nz * (nx * (ny - 1) + ny * (nx - 1))

def reduce_rows_kernel(g_ref, selt_ref, out_ref, give, acc, rc, ra1, rb1, ra2, rb2, rz, send, recv):
    p = Place()
    nz, nx, ny = p.nz, p.nx, p.ny
    rows = selt_ref.shape[1]
    half = rows // 2
    f32 = jnp.float32
    A, B = pl.ds(0, half), pl.ds(half, half)
    p.greet(p.line_peers())
    s, r = Pool(send), Pool(recv)
    sent = []
    slot = lambda dz, dx, dy: (dz * nx + dx) * ny + dy

    def push(src, dst, to):
        cp = pltpu.make_async_remote_copy(src_ref=src, dst_ref=dst, send_sem=s.take(), recv_sem=r.take(),
            device_id=p.dev(*to), device_id_type=MESH)
        cp.start()
        sent.append(cp)
        return cp

    zs = list(range(1, nz)) + [0]
    plane = [(dx, dy) for dx in reversed(range(nx)) for dy in reversed(range(ny))]
    cores, ca, cb, za, zb, zz = {}, {}, {}, {}, {}, {}

    def term(i):
        return jnp.dot(selt_ref[i], g_ref[i], preferred_element_type=f32)

    def stage_zero(dz):
        for dx, dy in plane:
            k = (dz, dx, dy)
            i = slot(*k)
            give[i] = term(p.index(*k, 1)).astype(give.dtype)
            cores[k] = push(give.at[i], rc.at[i], (0, 0, 0, 1))

    def add(dst, rows_, src):
        acc[dst, rows_, :] = (acc[dst, rows_, :].astype(f32) + src[...].astype(f32)).astype(acc.dtype)

    def stage_one(dz):
        for dx, dy in plane:
            k = (dz, dx, dy)
            i = slot(*k)
            mine = term(p.index(*k))
            cores[k].wait_recv()
            acc[i] = (mine + rc[i].astype(f32)).astype(acc.dtype)
            if dy:
                ca[k] = push(acc.at[i, A], ra1.at[dy - 1, dz * nx + dx], (0, 0, dy, 0))
            if dx:
                cb[k] = push(acc.at[i, B], rb1.at[dx - 1, dz * ny + dy], (0, dx, 0, 0))

    def stage_two(dz):
        for dx in reversed(range(nx)):
            for dy in range(1, ny):
                ca[dz, dx, dy].wait_recv()
                add(slot(dz, dx, 0), A, ra1.at[dy - 1, dz * nx + dx])
            if dx:
                za[dz, dx] = push(acc.at[slot(dz, dx, 0), A], ra2.at[dx - 1, dz], (0, dx, 0, 0))
        for dy in reversed(range(ny)):
            for dx in range(1, nx):
                cb[dz, dx, dy].wait_recv()
                add(slot(dz, 0, dy), B, rb1.at[dx - 1, dz * ny + dy])
            if dy:
                zb[dz, dy] = push(acc.at[slot(dz, 0, dy), B], rb2.at[dy - 1, dz], (0, 0, dy, 0))

    def stage_three(dz):
        for dx in range(1, nx):
            za[dz, dx].wait_recv()
            add(slot(dz, 0, 0), A, ra2.at[dx - 1, dz])
        for dy in range(1, ny):
            zb[dz, dy].wait_recv()
            add(slot(dz, 0, 0), B, rb2.at[dy - 1, dz])
        if dz:
            zz[dz] = push(acc.at[slot(dz, 0, 0)], rz.at[dz - 1], (dz, 0, 0, 0))

    stage_zero(zs[0])
    for k in range(nz + 2):
        if k + 1 < nz:
            stage_zero(zs[k + 1])
        if k < nz:
            stage_one(zs[k])
        if 0 <= k - 1 < nz:
            stage_two(zs[k - 1])
        if 0 <= k - 2 < nz:
            stage_three(zs[k - 2])
    total = acc[slot(0, 0, 0)].astype(f32)
    for dz in range(1, nz):
        zz[dz].wait_recv()
        total = total + rz[dz - 1].astype(f32)
    out_ref[...] = total
    for cp in sent:
        cp.wait_send()


def reduce_rows(made, select, cid):
    nz, nx, ny = grid_of()
    nd, cap, width = made.shape
    rows = select.shape[2]
    dt = made.dtype
    half = rows // 2
    n = 3 * nz * nx * ny + nz * (nx + ny) + nz
    blocks = 3 * nz * nx * ny + nz + (nz * (nx + 1) * (ny - 1) + nz * (ny + 1) * (nx - 1)) // 2 + 4
    parts = 1
    while (blocks * rows + nd * cap) * width * 2 // parts > 50 << 20:
        parts *= 2
    cols = width // parts
    one = pl.pallas_call(reduce_rows_kernel,
        out_shape=jax.ShapeDtypeStruct((rows, cols), jnp.float32),
        in_specs=[VM, VM], out_specs=VM,
        scratch_shapes=[pltpu.VMEM((nz * nx * ny, rows, cols), dt), pltpu.VMEM((nz * nx * ny, rows, cols), dt),
            pltpu.VMEM((nz * nx * ny, rows, cols), dt),
            pltpu.VMEM((ny - 1, nz * nx, half, cols), dt), pltpu.VMEM((nx - 1, nz * ny, half, cols), dt),
            pltpu.VMEM((nx - 1, nz, half, cols), dt), pltpu.VMEM((ny - 1, nz, half, cols), dt),
            pltpu.VMEM((nz - 1, rows, cols), dt),
            pltpu.SemaphoreType.DMA((n,)), pltpu.SemaphoreType.DMA((n,))],
        compiler_params=pltpu.CompilerParams(collective_id=cid, has_side_effects=True, vmem_limit_bytes=61 << 20),
        name="reduce_rows")
    turned = select.transpose(0, 2, 1)
    if parts == 1:
        return one(made, turned)
    return jnp.concatenate([one(made[:, :, k * cols:(k + 1) * cols], turned) for k in range(parts)], axis=1)


def expert_kernel(b_ref, sel_ref, selt_ref, gate_ref, g_ref, win_ref, wout_ref,
                  all_ref, in_ref, gr_ref, hid_ref, pg_ref, out_ref, back_ref,
                  xt, gt, in_t, gr_t, hid_t, pg_t, out_t, back_t, local_sem, x_sem, g_sem, store_sem, send, recv):
    p = Place()
    nz, nx, ny = p.nz, p.nx, p.ny
    ns = 2 * ny
    half = b_ref.shape[0] // 2
    cap = sel_ref.shape[1]
    size, width = wout_ref.shape
    f32, bf = jnp.float32, jnp.bfloat16
    A, B = pl.ds(0, half), pl.ds(half, half)
    F = pl.ds(0, 2 * half)
    p.greet(p.line_peers())
    own = pltpu.make_async_copy(b_ref, all_ref.at[p.index()], local_sem)
    own.start()
    s, r = Pool(send), Pool(recv)
    sent = []
    neg = lambda d, n: (n - d) % n

    def push(src_at, rows, to, first=False):
        i = p.index(*src_at)
        src = b_ref.at[rows] if first else all_ref.at[i, rows]
        cp = pltpu.make_async_remote_copy(src_ref=src, dst_ref=all_ref.at[i, rows], send_sem=s.take(),
            recv_sem=r.take(), device_id=p.dev(*to), device_id_type=MESH)
        cp.start()
        sent.append(cp)
        return cp

    first = {d: push((0, 0, 0, 0), F, (d, 0, 0, 0), True) for d in range(1, nz)}
    second_a, second_b, third, other = {}, {}, {}, {}

    def cross(at, rows, is_first=False):
        dx = neg(at[1], nx)
        other.setdefault((neg(at[0], nz), dx), []).append(push(at, rows, (0, 0, 0, 1), is_first))

    def stage_one(k):
        if k:
            first[k].wait_recv()
        at = (neg(k, nz), 0, 0, 0)
        for d in range(1, nx):
            second_a[k, d] = push(at, A, (0, d, 0, 0), k == 0)
        for d in range(1, ny):
            second_b[k, d] = push(at, B, (0, 0, d, 0), k == 0)
        for d in range(1, ny):
            third["a", k, 0, d] = push(at, A, (0, 0, d, 0), k == 0)
        for d in range(1, nx):
            third["b", k, 0, d] = push(at, B, (0, d, 0, 0), k == 0)
        cross(at, F, k == 0)

    def stage_two(k):
        for dx in range(1, nx):
            second_a[k, dx].wait_recv()
            at = (neg(k, nz), neg(dx, nx), 0, 0)
            for d in range(1, ny):
                third["a", k, dx, d] = push(at, A, (0, 0, d, 0))
            cross(at, A)
        for dy in range(1, ny):
            second_b[k, dy].wait_recv()
            at = (neg(k, nz), 0, neg(dy, ny), 0)
            for d in range(1, nx):
                third["b", k, dy, d] = push(at, B, (0, d, 0, 0))
            cross(at, B)

    def stage_three(k):
        for dx in range(nx):
            for d in range(1, ny):
                third["a", k, dx, d].wait_recv()
                cross((neg(k, nz), neg(dx, nx), neg(d, ny), 0), A)
        for dy in range(ny):
            for d in range(1, nx):
                third["b", k, dy, d].wait_recv()
                cross((neg(k, nz), neg(d, nx), neg(dy, ny), 0), B)

    whole = nx * ns <= 8
    groups = [(k, None) for k in range(nz)] if whole else [(k, dx) for k in range(nz) for dx in range(nx)]
    gb = nx * ns if whole else ns

    def base_of(i):
        k, dx = groups[i]
        z, x, _, _ = p.at(neg(k, nz), neg(dx or 0, nx), 0, 0)
        return z * nx * ns if whole else (z * nx + x) * ns

    def load_x(i):
        return pltpu.make_async_copy(all_ref.at[pl.ds(base_of(i), gb)], xt, x_sem)

    def load_g(i):
        return pltpu.make_async_copy(g_ref.at[pl.ds(base_of(i), gb)], gt.at[i % 2], g_sem.at[i % 2])

    def stores(i, part):
        rows = pl.ds(base_of(i) * cap, gb * cap)
        pairs = [[(in_t, in_ref.at[rows]), (gr_t, gr_ref.at[rows])], [(hid_t, hid_ref.at[rows]), (pg_t, pg_ref.at[rows])],
            [(out_t, out_ref.at[pl.ds(base_of(i), gb)]), (back_t, back_ref.at[rows])]][part]
        return [pltpu.make_async_copy(a, b, store_sem.at[part, j]) for j, (a, b) in enumerate(pairs)]

    def compute(i):
        load_x(i).start()
        if i + 1 < len(groups):
            load_g(i + 1).start()
        load_g(i).wait()
        base = base_of(i)
        if i:
            for cp in stores(i - 1, 0):
                cp.wait()
        load_x(i).wait()

        def pick(b, carry):
            rows = pl.ds(pl.multiple_of(b * cap, cap), cap)
            sel = sel_ref[base + b]
            in_t[rows, :] = jnp.dot(sel, xt[b], preferred_element_type=f32).astype(bf)
            gr_t[rows, :] = (jnp.dot(sel, gt[i % 2, b], preferred_element_type=f32) * gate_ref[base + b][:, :1]).astype(bf)
            return carry

        lax.fori_loop(0, gb, pick, 0)
        for cp in stores(i, 0):
            cp.start()
        if i:
            for cp in stores(i - 1, 1):
                cp.wait()
        wide = min(size, 256)

        def middle(j, carry):
            left = pl.ds(pl.multiple_of(j * wide, wide), wide)
            right = pl.ds(pl.multiple_of(size + j * wide, wide), wide)
            rows_in, rows_grad = in_t[...], gr_t[...]
            a = jnp.dot(rows_in, win_ref[:, left], preferred_element_type=f32)
            b = jnp.dot(rows_in, win_ref[:, right], preferred_element_type=f32)
            h = lax.dot_general(rows_grad, wout_ref[left, :], (((1,), (1,)), ((), ())), preferred_element_type=f32)
            sigma = 1.0 / (1.0 + jnp.exp(-a))
            active = a * sigma
            hid_t[:, left] = (active * b).astype(bf)
            pg_t[:, left] = (h * b * (sigma * (1.0 + a * (1.0 - sigma)))).astype(bf)
            pg_t[:, right] = (h * active).astype(bf)
            return carry

        lax.fori_loop(0, size // wide, middle, 0)
        for cp in stores(i, 1):
            cp.start()
        if i:
            for cp in stores(i - 1, 2):
                cp.wait()
        gates = jnp.concatenate([gate_ref[base + b][:, :1] for b in range(gb)], axis=0)

        def final(j, carry):
            cols = pl.ds(pl.multiple_of(j * 256, 256), 256)
            out = jnp.dot(hid_t[...], wout_ref[:, cols], preferred_element_type=f32).astype(bf)
            weighted = (out.astype(f32) * gates).astype(bf)
            back_t[:, cols] = lax.dot_general(pg_t[...], win_ref[cols, :], (((1,), (1,)), ((), ())),
                preferred_element_type=f32).astype(bf)
            for b in range(gb):
                out_t[b, :, cols] = jnp.dot(selt_ref[base + b], weighted[b * cap:(b + 1) * cap],
                    preferred_element_type=f32).astype(bf)
            return carry

        lax.fori_loop(0, width // 256, final, 0)
        for cp in stores(i, 2):
            cp.start()

    load_g(0).start()
    for k in range(nz + 2):
        if k < nz:
            stage_one(k)
        if 0 <= k - 1 < nz:
            stage_two(k - 1)
        if 0 <= k - 2 < nz:
            stage_three(k - 2)
            if k == 2:
                own.wait()
            for i, (z_group, dx) in enumerate(groups):
                if z_group == k - 2:
                    for each in (range(nx) if whole else [dx]):
                        for cp in other[k - 2, each]:
                            cp.wait_recv()
                    compute(i)
    for part in range(3):
        for cp in stores(len(groups) - 1, part):
            cp.wait()
    for cp in sent:
        cp.wait_send()


def expert_pass(block, select, gate, grads_all, w_in, w_out, cid):
    nz, nx, ny = grid_of()
    nd, ns = nz * nx * ny * 2, ny * 2
    rows, width = block.shape
    cap, size = select.shape[1], w_out.shape[0]
    bf = jnp.bfloat16
    n = n_sems(nz, nx, ny)
    made = nd * cap
    gb = nx * ns if nx * ns <= 8 else ns
    tile = gb * cap
    sds = jax.ShapeDtypeStruct
    results = pl.pallas_call(expert_kernel,
        out_shape=(sds((nd, rows, width), bf), sds((made, width), bf), sds((made, width), bf), sds((made, size), bf),
            sds((made, 2 * size), bf), sds((nd, rows, width), bf), sds((made, width), bf)),
        in_specs=[VM, VM, VM, VM, ANY, VM, VM], out_specs=(ANY,) * 7,
        scratch_shapes=[pltpu.VMEM((gb, rows, width), bf), pltpu.VMEM((2, gb, rows, width), bf),
            pltpu.VMEM((tile, width), bf), pltpu.VMEM((tile, width), bf), pltpu.VMEM((tile, size), bf),
            pltpu.VMEM((tile, 2 * size), bf), pltpu.VMEM((gb, rows, width), bf), pltpu.VMEM((tile, width), bf),
            pltpu.SemaphoreType.DMA, pltpu.SemaphoreType.DMA, pltpu.SemaphoreType.DMA((2,)),
            pltpu.SemaphoreType.DMA((3, 2)), pltpu.SemaphoreType.DMA((n,)), pltpu.SemaphoreType.DMA((n,))],
        compiler_params=pltpu.CompilerParams(collective_id=cid, has_side_effects=True, vmem_limit_bytes=61 << 20),
        name="expert_pass")(block, select, select.transpose(0, 2, 1), jnp.broadcast_to(gate[:, :, None], gate.shape + (128,)),
            grads_all, w_in, w_out)
    return results[1:]


def expert_reduce_kernel(b_ref, sel_ref, selt_ref, gate_ref, g_ref, win_ref, wout_ref,
                         all_ref, in_ref, gr_ref, hid_ref, pg_ref, out_ref, sum_ref,
                         xt, gt, in_t, gr_t, hid_t, pg_t, out_t, back_t, give, acc, rc, ra1, rb1, ra2, rb2, rz,
                         local_sem, x_sem, g_sem, store_sem, out_sem, send, recv):
    p = Place()
    nz, nx, ny = p.nz, p.nx, p.ny
    ns = 2 * ny
    half = b_ref.shape[0] // 2
    cap = sel_ref.shape[1]
    size, width = wout_ref.shape
    f32, bf = jnp.float32, jnp.bfloat16
    A, B = pl.ds(0, half), pl.ds(half, half)
    F = pl.ds(0, 2 * half)
    p.greet(p.line_peers())
    own = pltpu.make_async_copy(b_ref, all_ref.at[p.index()], local_sem)
    own.start()
    s, r = Pool(send), Pool(recv)
    sent = []
    neg = lambda d, n: (n - d) % n

    def push(src_at, rows, to, first=False):
        i = p.index(*src_at)
        src = b_ref.at[rows] if first else all_ref.at[i, rows]
        cp = pltpu.make_async_remote_copy(src_ref=src, dst_ref=all_ref.at[i, rows], send_sem=s.take(),
            recv_sem=r.take(), device_id=p.dev(*to), device_id_type=MESH)
        cp.start()
        sent.append(cp)
        return cp

    first = {d: push((0, 0, 0, 0), F, (d, 0, 0, 0), True) for d in range(1, nz)}
    second_a, second_b, third, other = {}, {}, {}, {}

    def cross(at, rows, is_first=False):
        dx = neg(at[1], nx)
        other.setdefault((neg(at[0], nz), dx), []).append(push(at, rows, (0, 0, 0, 1), is_first))

    def stage_one(k):
        if k:
            first[k].wait_recv()
        at = (neg(k, nz), 0, 0, 0)
        for d in range(1, nx):
            second_a[k, d] = push(at, A, (0, d, 0, 0), k == 0)
        for d in range(1, ny):
            second_b[k, d] = push(at, B, (0, 0, d, 0), k == 0)
        for d in range(1, ny):
            third["a", k, 0, d] = push(at, A, (0, 0, d, 0), k == 0)
        for d in range(1, nx):
            third["b", k, 0, d] = push(at, B, (0, d, 0, 0), k == 0)
        cross(at, F, k == 0)

    def stage_two(k):
        for dx in range(1, nx):
            second_a[k, dx].wait_recv()
            at = (neg(k, nz), neg(dx, nx), 0, 0)
            for d in range(1, ny):
                third["a", k, dx, d] = push(at, A, (0, 0, d, 0))
            cross(at, A)
        for dy in range(1, ny):
            second_b[k, dy].wait_recv()
            at = (neg(k, nz), 0, neg(dy, ny), 0)
            for d in range(1, nx):
                third["b", k, dy, d] = push(at, B, (0, d, 0, 0))
            cross(at, B)

    def stage_three(k):
        for dx in range(nx):
            for d in range(1, ny):
                third["a", k, dx, d].wait_recv()
                cross((neg(k, nz), neg(dx, nx), neg(d, ny), 0), A)
        for dy in range(ny):
            for d in range(1, nx):
                third["b", k, dy, d].wait_recv()
                cross((neg(k, nz), neg(d, nx), neg(dy, ny), 0), B)

    gb = nx * ns

    def base_of(i):
        return p.at(neg(i, nz), 0, 0, 0)[0] * gb

    def load_x(i):
        return pltpu.make_async_copy(all_ref.at[pl.ds(base_of(i), gb)], xt, x_sem)

    def load_g(i):
        return pltpu.make_async_copy(g_ref.at[pl.ds(base_of(i), gb)], gt, g_sem)

    def stores(i, part):
        rows = pl.ds(base_of(i) * cap, gb * cap)
        pairs = [[(in_t, in_ref.at[rows]), (gr_t, gr_ref.at[rows])], [(hid_t, hid_ref.at[rows]), (pg_t, pg_ref.at[rows])]][part]
        return [pltpu.make_async_copy(a, b, store_sem.at[part, j]) for j, (a, b) in enumerate(pairs)]

    def compute(i):
        load_x(i).start()
        load_g(i).wait()
        base = base_of(i)
        if i:
            for cp in stores(i - 1, 0):
                cp.wait()
        load_x(i).wait()

        def pick(b, carry):
            rows = pl.ds(pl.multiple_of(b * cap, cap), cap)
            sel = sel_ref[base + b]
            in_t[rows, :] = jnp.dot(sel, xt[b], preferred_element_type=f32).astype(bf)
            gr_t[rows, :] = (jnp.dot(sel, gt[b], preferred_element_type=f32) * gate_ref[base + b][:, :1]).astype(bf)
            return carry

        lax.fori_loop(0, gb, pick, 0)
        if i + 1 < nz:
            load_g(i + 1).start()
        for cp in stores(i, 0):
            cp.start()
        if i:
            for cp in stores(i - 1, 1):
                cp.wait()
        wide = min(size, 256)

        def middle(j, carry):
            left = pl.ds(pl.multiple_of(j * wide, wide), wide)
            right = pl.ds(pl.multiple_of(size + j * wide, wide), wide)
            rows_in, rows_grad = in_t[...], gr_t[...]
            a = jnp.dot(rows_in, win_ref[:, left], preferred_element_type=f32)
            b = jnp.dot(rows_in, win_ref[:, right], preferred_element_type=f32)
            h = lax.dot_general(rows_grad, wout_ref[left, :], (((1,), (1,)), ((), ())), preferred_element_type=f32)
            sigma = 1.0 / (1.0 + jnp.exp(-a))
            active = a * sigma
            hid_t[:, left] = (active * b).astype(bf)
            pg_t[:, left] = (h * b * (sigma * (1.0 + a * (1.0 - sigma)))).astype(bf)
            pg_t[:, right] = (h * active).astype(bf)
            return carry

        lax.fori_loop(0, size // wide, middle, 0)
        for cp in stores(i, 1):
            cp.start()
        gates = jnp.concatenate([gate_ref[base + b][:, :1] for b in range(gb)], axis=0)

        def out_copy(j):
            t = lax.rem(j, 2)
            cols = pl.ds(pl.multiple_of(j * 256, 256), 256)
            return pltpu.make_async_copy(out_t.at[t], out_ref.at[pl.ds(base, gb), :, cols], out_sem.at[t])

        def final(j, carry):
            cols = pl.ds(pl.multiple_of(j * 256, 256), 256)
            out = jnp.dot(hid_t[...], wout_ref[:, cols], preferred_element_type=f32).astype(bf)
            weighted = (out.astype(f32) * gates).astype(bf)
            back_t[:, cols] = lax.dot_general(pg_t[...], win_ref[cols, :], (((1,), (1,)), ((), ())),
                preferred_element_type=f32).astype(bf)

            @pl.when(j >= 2)
            def _():
                out_copy(j - 2).wait()

            for b in range(gb):
                out_t[lax.rem(j, 2), b] = jnp.dot(selt_ref[base + b], weighted[b * cap:(b + 1) * cap],
                    preferred_element_type=f32).astype(bf)
            out_copy(j).start()
            return carry

        steps = width // 256
        lax.fori_loop(0, steps, final, 0)
        for j in range(max(0, steps - 2), steps):
            out_copy(j).wait()

    plane = [(dx, dy) for dx in reversed(range(nx)) for dy in reversed(range(ny))]
    slot = lambda dz, dx, dy: (dz * nx + dx) * ny + dy
    cores, ca, cb, za, zb, zz = {}, {}, {}, {}, {}, {}
    done = []

    def push_to(src, dst, to):
        cp = pltpu.make_async_remote_copy(src_ref=src, dst_ref=dst, send_sem=s.take(), recv_sem=r.take(),
            device_id=p.dev(*to), device_id_type=MESH)
        cp.start()
        sent.append(cp)
        return cp

    def term(i, index):
        b = index - base_of(i)
        rows = pl.ds(pl.multiple_of(b * cap, cap), cap)
        return jnp.dot(selt_ref[index], back_t[rows, :], preferred_element_type=f32)

    def add(dst, rows_, src):
        acc[dst, rows_, :] = (acc[dst, rows_, :].astype(f32) + src[...].astype(f32)).astype(acc.dtype)

    def sum_one(i):
        dz = neg(i, nz)
        for j, (dx, dy) in enumerate(plane):
            g = (i % 2) * len(plane) + j
            if i >= 2:
                old = cores[neg(i - 2, nz), dx, dy]
                old.wait_send()
                done.append(old)
            give[g] = term(i, p.index(dz, dx, dy, 1)).astype(bf)
            cores[dz, dx, dy] = push_to(give.at[g], rc.at[slot(dz, dx, dy)], (0, 0, 0, 1))
        for dx, dy in plane:
            t = slot(dz, dx, dy)
            mine = term(i, p.index(dz, dx, dy))
            cores[dz, dx, dy].wait_recv()
            acc[t] = (mine + rc[t].astype(f32)).astype(bf)
            if dy:
                ca[dz, dx, dy] = push_to(acc.at[t, A], ra1.at[dy - 1, dz * nx + dx], (0, 0, dy, 0))
            if dx:
                cb[dz, dx, dy] = push_to(acc.at[t, B], rb1.at[dx - 1, dz * ny + dy], (0, dx, 0, 0))

    def sum_two(i):
        dz = neg(i, nz)
        for dx in reversed(range(nx)):
            for dy in range(1, ny):
                ca[dz, dx, dy].wait_recv()
                add(slot(dz, dx, 0), A, ra1.at[dy - 1, dz * nx + dx])
            if dx:
                za[dz, dx] = push_to(acc.at[slot(dz, dx, 0), A], ra2.at[dx - 1, dz], (0, dx, 0, 0))
        for dy in reversed(range(ny)):
            for dx in range(1, nx):
                cb[dz, dx, dy].wait_recv()
                add(slot(dz, 0, dy), B, rb1.at[dx - 1, dz * ny + dy])
            if dy:
                zb[dz, dy] = push_to(acc.at[slot(dz, 0, dy), B], rb2.at[dy - 1, dz], (0, 0, dy, 0))

    def sum_three(i):
        dz = neg(i, nz)
        for dx in range(1, nx):
            za[dz, dx].wait_recv()
            add(slot(dz, 0, 0), A, ra2.at[dx - 1, dz])
        for dy in range(1, ny):
            zb[dz, dy].wait_recv()
            add(slot(dz, 0, 0), B, rb2.at[dy - 1, dz])
        if dz:
            zz[dz] = push_to(acc.at[slot(dz, 0, 0)], rz.at[dz - 1], (dz, 0, 0, 0))

    load_g(0).start()
    for k in range(nz + 2):
        if k < nz:
            stage_one(k)
        if 0 <= k - 1 < nz:
            stage_two(k - 1)
        if 0 <= k - 2 < nz:
            stage_three(k - 2)
            if k == 2:
                own.wait()
            for dx in range(nx):
                for cp in other[k - 2, dx]:
                    cp.wait_recv()
            compute(k - 2)
            sum_one(k - 2)
            if k - 3 >= 0:
                sum_two(k - 3)
            if k - 4 >= 0:
                sum_three(k - 4)
    sum_two(nz - 1)
    for i in range(max(0, nz - 2), nz):
        sum_three(i)
    total = acc[slot(0, 0, 0)].astype(f32)
    for dz in range(1, nz):
        zz[dz].wait_recv()
        total = total + rz[dz - 1].astype(f32)
    sum_ref[...] = total
    for part in range(2):
        for cp in stores(nz - 1, part):
            cp.wait()
    for cp in sent:
        if not any(cp is other_cp for other_cp in done):
            cp.wait_send()


def expert_reduce(block, select, gate, grads_all, w_in, w_out, cid):
    nz, nx, ny = grid_of()
    nd, gb = nz * nx * ny * 2, nx * ny * 2
    rows, width = block.shape
    half = rows // 2
    cap, size = select.shape[1], w_out.shape[0]
    bf = jnp.bfloat16
    n = n_sems(nz, nx, ny) + 2 * nz * nx * ny + nz * (nx + ny) + 2 * nz * (nx * (ny - 1) + ny * (nx - 1))
    made, tile, slots = nd * cap, gb * cap, nz * nx * ny
    sds = jax.ShapeDtypeStruct
    results = pl.pallas_call(expert_reduce_kernel,
        out_shape=(sds((nd, rows, width), bf), sds((made, width), bf), sds((made, width), bf), sds((made, size), bf),
            sds((made, 2 * size), bf), sds((nd, rows, width), bf), sds((rows, width), jnp.float32)),
        in_specs=[VM, VM, VM, VM, ANY, VM, VM], out_specs=(ANY,) * 6 + (VM,),
        scratch_shapes=[pltpu.VMEM((gb, rows, width), bf), pltpu.VMEM((gb, rows, width), bf),
            pltpu.VMEM((tile, width), bf), pltpu.VMEM((tile, width), bf), pltpu.VMEM((tile, size), bf),
            pltpu.VMEM((tile, 2 * size), bf), pltpu.VMEM((2, gb, rows, 256), bf), pltpu.VMEM((tile, width), bf),
            pltpu.VMEM((2 * nx * ny, rows, width), bf), pltpu.VMEM((slots, rows, width), bf), pltpu.VMEM((slots, rows, width), bf),
            pltpu.VMEM((ny - 1, nz * nx, half, width), bf), pltpu.VMEM((nx - 1, nz * ny, half, width), bf),
            pltpu.VMEM((nx - 1, nz, half, width), bf), pltpu.VMEM((ny - 1, nz, half, width), bf),
            pltpu.VMEM((nz - 1, rows, width), bf),
            pltpu.SemaphoreType.DMA, pltpu.SemaphoreType.DMA, pltpu.SemaphoreType.DMA,
            pltpu.SemaphoreType.DMA((2, 2)), pltpu.SemaphoreType.DMA((2,)),
            pltpu.SemaphoreType.DMA((n,)), pltpu.SemaphoreType.DMA((n,))],
        compiler_params=pltpu.CompilerParams(collective_id=cid, has_side_effects=True, vmem_limit_bytes=67043328),
        name="expert_reduce")(block, select, select.transpose(0, 2, 1), jnp.broadcast_to(gate[:, :, None], gate.shape + (128,)),
            grads_all, w_in, w_out)
    return results[1:]


def shard_peers(ny):
    return [(0, 0, dy, dc) for dy in range(ny) for dc in range(2) if dy or dc]


def weights_kernel(w_ref, wo_ref, t_ref, wall_ref, woall_ref, tall_ref, local_sem, send, recv):
    p = Place()
    nz, nx, ny = p.nz, p.nx, p.ny
    ns = ny * 2
    e, sh = lax.axis_index("expert"), lax.axis_index("shard")
    ne = nz * nx
    me = e * ns + sh
    to_e, to_s = me % ne, me // ne
    from_e, from_s = (sh * ne + e) // ns, (sh * ne + e) % ns
    moved = jnp.logical_not(jnp.logical_and(to_e == e, to_s == sh))
    peers = [q for q in p.line_peers() if not (q[2] or q[3])] + shard_peers(ny)
    barrier = pltpu.get_barrier_semaphore()
    for q in peers:
        pl.semaphore_signal(barrier, inc=1, device_id=p.dev(*q), device_id_type=MESH)

    @pl.when(moved)
    def _():
        pl.semaphore_signal(barrier, inc=1, device_id=(from_e, from_s), device_id_type=MESH)

    pl.semaphore_wait(barrier, len(peers) + moved.astype(jnp.int32))
    s, r = Pool(send), Pool(recv)
    sent = []
    neg = lambda d, n: (n - d) % n

    def push(src, dst, to):
        cp = pltpu.make_async_remote_copy(src_ref=src, dst_ref=dst, send_sem=s.take(), recv_sem=r.take(),
            device_id=p.dev(*to), device_id_type=MESH)
        cp.start()
        sent.append(cp)
        return cp

    mixed = []
    for q in shard_peers(ny):
        _, _, y, c = p.at(*q)
        mixed.append(push(w_ref.at[y * 2 + c], wall_ref.at[me], q))
    own_w = pltpu.make_async_copy(w_ref.at[sh], wall_ref.at[me], local_sem.at[0])
    own_w.start()
    entry_send, entry_recv = s.take(), r.take()
    entry = pltpu.make_async_remote_copy(src_ref=wo_ref, dst_ref=woall_ref.at[to_e], send_sem=entry_send,
        recv_sem=entry_recv, device_id=(to_e, to_s), device_id_type=MESH)
    stay = pltpu.make_async_copy(wo_ref, woall_ref.at[e], local_sem.at[1])

    @pl.when(moved)
    def _():
        entry.start()

    @pl.when(jnp.logical_not(moved))
    def _():
        stay.start()

    own_t = pltpu.make_async_copy(t_ref, tall_ref.at[sh], local_sem.at[2])
    own_t.start()
    toks = {}
    for d in range(1, ny):
        toks[d] = push(t_ref, tall_ref.at[sh], (0, 0, d, 0))
    tail = [push(t_ref, tall_ref.at[sh], (0, 0, 0, 1))]

    def block(ref, zz, size):
        z, x, _, _ = p.at(zz, 0, 0, 0)
        return ref.at[pl.ds((z * nx + x) * size, size)]

    def spread_first(ref, size):
        lines = {}
        for d in range(1, nz):
            b = block(ref, 0, size)
            lines[d] = push(b, b, (d, 0, 0, 0))
        for d in range(1, nx):
            b = block(ref, 0, size)
            tail.append(push(b, b, (0, d, 0, 0)))
        return lines

    def spread_next(ref, size, lines, d):
        lines[d].wait_recv()
        for dx in range(1, nx):
            b = block(ref, neg(d, nz), size)
            tail.append(push(b, b, (0, dx, 0, 0)))

    own_w.wait()
    for cp in mixed:
        cp.wait_recv()
    lines_w = spread_first(wall_ref, ns)

    @pl.when(moved)
    def _():
        entry.wait()

    @pl.when(jnp.logical_not(moved))
    def _():
        stay.wait()

    lines_o = spread_first(woall_ref, 1)
    for d in range(1, ny):
        toks[d].wait_recv()
        _, _, y, c = p.at(0, 0, neg(d, ny), 0)
        b = tall_ref.at[y * 2 + c]
        tail.append(push(b, b, (0, 0, 0, 1)))
    for d in range(1, nz):
        spread_next(wall_ref, ns, lines_w, d)
    for d in range(1, nz):
        spread_next(woall_ref, 1, lines_o, d)
    for cp in tail:
        cp.wait_recv()
    for cp in sent:
        cp.wait_send()
    own_t.wait()


def gather_weights(w, wo, t, cid):
    nz, nx, ny = grid_of()
    ns, ne = ny * 2, nz * nx
    n = 2 * ns + 2 + 2 * (nz + nx + nz * nx) + 2 * ny + 8
    return pl.pallas_call(weights_kernel,
        out_shape=(jax.ShapeDtypeStruct((ne * ns,) + w.shape[1:], w.dtype),
            jax.ShapeDtypeStruct((ne,) + wo.shape, wo.dtype), jax.ShapeDtypeStruct((ns,) + t.shape, t.dtype)),
        in_specs=[VM, VM, VM], out_specs=(ANY, ANY, ANY),
        scratch_shapes=[pltpu.SemaphoreType.DMA((3,)), pltpu.SemaphoreType.DMA((n,)), pltpu.SemaphoreType.DMA((n,))],
        compiler_params=pltpu.CompilerParams(collective_id=cid, has_side_effects=True),
        name="gather_weights")(w, wo, t)


def pack_gather_kernel(t_ref, o_ref, local_sem, send, recv):
    p = Place()
    ny = p.ny
    p.greet([(0, 0, d, 0) for d in range(1, ny)] + [(0, 0, 0, 1)])
    sh = lax.axis_index("shard")
    own = pltpu.make_async_copy(t_ref, o_ref.at[sh], local_sem)
    own.start()
    s, r = Pool(send), Pool(recv)
    sent, tail, along = [], [], {}
    rows = t_ref.shape[0]
    pieces = 4

    def push(src, dst, to):
        cp = pltpu.make_async_remote_copy(src_ref=src, dst_ref=dst, send_sem=s.take(), recv_sem=r.take(),
            device_id=p.dev(*to), device_id_type=MESH)
        cp.start()
        sent.append(cp)
        return cp

    part = [pl.ds(k * (rows // pieces), rows // pieces) for k in range(pieces)]
    for k in range(pieces):
        for d in range(1, ny):
            along[k, d] = push(t_ref.at[part[k]], o_ref.at[sh, part[k]], (0, 0, d, 0))
    tail.append(push(t_ref, o_ref.at[sh], (0, 0, 0, 1)))
    for k in range(pieces):
        for d in range(1, ny):
            along[k, d].wait_recv()
            _, _, y, c = p.at(0, 0, (ny - d) % ny, 0)
            b = o_ref.at[y * 2 + c, part[k]]
            tail.append(push(b, b, (0, 0, 0, 1)))
    for cp in tail:
        cp.wait_recv()
    for cp in sent:
        cp.wait_send()
    own.wait()


def pack_gather(t, cid):
    nz, nx, ny = grid_of()
    n = 8 * ny
    return pl.pallas_call(pack_gather_kernel,
        out_shape=jax.ShapeDtypeStruct((ny * 2,) + t.shape, t.dtype), in_specs=[VM], out_specs=VM,
        scratch_shapes=[pltpu.SemaphoreType.DMA, pltpu.SemaphoreType.DMA((n,)), pltpu.SemaphoreType.DMA((n,))],
        compiler_params=pltpu.CompilerParams(collective_id=cid, has_side_effects=True),
        name="pack_gather")(t)


def pack_reduce_body(p, g_ref, out_ref, acc, rc, ry, push, pieces=4):
    ny = p.ny
    rows = g_ref.shape[1]
    step = rows // pieces
    part = [pl.ds(k * step, step) for k in range(pieces)]
    order = list(range(1, ny)) + [0]
    cores, along = {}, {}
    for k in range(pieces):
        for dy in order:
            _, _, y, c = p.at(0, 0, dy, 1)
            cores[k, dy] = push(g_ref.at[y * 2 + c, part[k]], rc.at[dy, part[k]], (0, 0, 0, 1))

    def first():
        for k in range(pieces):
            for dy in order:
                _, _, y, c = p.at(0, 0, dy, 0)
                cores[k, dy].wait_recv()
                both = g_ref[y * 2 + c, part[k], :].astype(jnp.float32) + rc[dy, part[k], :].astype(jnp.float32)
                if dy:
                    acc[dy - 1, part[k], :] = both.astype(acc.dtype)
                    along[k, dy] = push(acc.at[dy - 1, part[k]], ry.at[dy - 1, part[k]], (0, 0, dy, 0))
                else:
                    out_ref[part[k], :] = both

    def second():
        for k in range(pieces):
            for dy in range(1, ny):
                along[k, dy].wait_recv()
                out_ref[part[k], :] = out_ref[part[k], :] + ry[dy - 1, part[k], :].astype(jnp.float32)

    return first, second


def pack_reduce_kernel(g_ref, out_ref, acc, rc, ry, send, recv):
    p = Place()
    p.greet([(0, 0, d, 0) for d in range(1, p.ny)] + [(0, 0, 0, 1)])
    s, r = Pool(send), Pool(recv)
    sent = []

    def push(src, dst, to):
        cp = pltpu.make_async_remote_copy(src_ref=src, dst_ref=dst, send_sem=s.take(), recv_sem=r.take(),
            device_id=p.dev(*to), device_id_type=MESH)
        cp.start()
        sent.append(cp)
        return cp

    first, second = pack_reduce_body(p, g_ref, out_ref, acc, rc, ry, push)
    first()
    second()
    for cp in sent:
        cp.wait_send()


def pack_scratch(ny, rows, width, dt):
    return [pltpu.VMEM((ny - 1, rows, width), dt), pltpu.VMEM((ny, rows, width), dt), pltpu.VMEM((ny - 1, rows, width), dt)]


def pack_reduce(terms, cid):
    nz, nx, ny = grid_of()
    ns, rows, width = terms.shape
    n = 8 * ny
    return pl.pallas_call(pack_reduce_kernel,
        out_shape=jax.ShapeDtypeStruct((rows, width), jnp.float32), in_specs=[VM], out_specs=VM,
        scratch_shapes=pack_scratch(ny, rows, width, terms.dtype)
            + [pltpu.SemaphoreType.DMA((n,)), pltpu.SemaphoreType.DMA((n,))],
        compiler_params=pltpu.CompilerParams(collective_id=cid, has_side_effects=True, vmem_limit_bytes=40 << 20),
        name="pack_reduce")(terms)


def grads_kernel(wo_ref, w_ref, s_ref, n_ref, wo_out, w_out, s_out, n_out,
                 wo_x, wo_z, wo_l, wo_r, w_x, w_z, w_l, w_r, s_x, s_z, s_l, acc, rc, ry, load_sem, send, recv):
    p = Place()
    nz, nx, ny = p.nz, p.nx, p.ny
    ns, ne = ny * 2, nz * nx
    e, sh = lax.axis_index("expert"), lax.axis_index("shard")
    me = e * ns + sh
    own_e, own_s = (sh * ne + e) // ns, (sh * ne + e) % ns
    from_e, from_s = me % ne, me // ne
    moved = jnp.logical_not(jnp.logical_and(own_e == e, own_s == sh))
    peers = [q for q in p.line_peers() if not (q[2] or q[3])] + shard_peers(ny)
    barrier = pltpu.get_barrier_semaphore()
    for q in peers:
        pl.semaphore_signal(barrier, inc=1, device_id=p.dev(*q), device_id_type=MESH)

    @pl.when(moved)
    def _():
        pl.semaphore_signal(barrier, inc=1, device_id=(from_e, from_s), device_id_type=MESH)

    pl.semaphore_wait(barrier, len(peers) + moved.astype(jnp.int32))
    s, r = Pool(send), Pool(recv)
    sent = []

    def push(src, dst, to):
        cp = pltpu.make_async_remote_copy(src_ref=src, dst_ref=dst, send_sem=s.take(), recv_sem=r.take(),
            device_id=p.dev(*to), device_id_type=MESH)
        cp.start()
        sent.append(cp)
        return cp

    zs = list(range(1, nz)) + [0]
    jobs = [(w_ref, w_x, w_z, w_l, ns, 0), (s_ref, s_x, s_z, s_l, ns, nz), (wo_ref, wo_x, wo_z, wo_l, 1, 2 * nz)]

    def group(ref, dz, dx, size):
        z, x, _, _ = p.at(dz, dx, 0, 0)
        return ref.at[pl.ds((z * nx + x) * size, size)]

    xs, loads, lines = {}, {}, {}
    for j, (ref, x_buf, z_buf, l_buf, size, base) in enumerate(jobs):
        for dz in zs:
            for dx in range(1, nx):
                xs[j, dz, dx] = push(group(ref, dz, dx, size), x_buf.at[dx - 1, dz], (0, dx, 0, 0))
            loads[j, dz] = pltpu.make_async_copy(group(ref, dz, 0, size), l_buf.at[dz], load_sem.at[base + dz])
            loads[j, dz].start()
    first, second = pack_reduce_body(p, n_ref, n_out, acc, rc, ry, push)
    first()
    for j, (ref, x_buf, z_buf, l_buf, size, base) in enumerate(jobs):
        for dz in zs:
            loads[j, dz].wait()
            for dx in range(1, nx):
                xs[j, dz, dx].wait_recv()
            total = l_buf[dz].astype(jnp.float32)
            for dx in range(1, nx):
                total = total + x_buf[dx - 1, dz].astype(jnp.float32)
            l_buf[dz] = total.astype(l_buf.dtype)
            if dz:
                lines[j, dz] = push(l_buf.at[dz], z_buf.at[dz - 1], (dz, 0, 0, 0))
    second()
    last = []
    entry = pltpu.make_async_remote_copy(src_ref=wo_l.at[0, 0], dst_ref=wo_r, send_sem=s.take(),
        recv_sem=r.take(), device_id=(own_e, own_s), device_id_type=MESH)
    for j, (ref, x_buf, z_buf, l_buf, size, base) in enumerate(jobs):
        total = l_buf[0].astype(jnp.float32)
        for d in range(1, nz):
            lines[j, d].wait_recv()
            total = total + z_buf[d - 1].astype(jnp.float32)
        l_buf[0] = total.astype(l_buf.dtype)
        if j == 0:
            for q in shard_peers(ny):
                _, _, y, c = p.at(*q)
                last.append(push(l_buf.at[0, y * 2 + c], w_r.at[sh], q))
            w_r[sh] = l_buf[0, sh]
        elif j == 1:
            for q in shard_peers(ny):
                _, _, y, c = p.at(*q)
                last.append(push(l_buf.at[0, y * 2 + c], s_out.at[sh], q))
            s_out[sh] = l_buf[0, sh]

    @pl.when(moved)
    def _():
        entry.start()

    for cp in last:
        cp.wait_recv()
    w_out[...] = w_r[...].astype(jnp.float32)

    @pl.when(moved)
    def _():
        entry.wait()
        wo_out[...] = wo_r[...].astype(jnp.float32)

    @pl.when(jnp.logical_not(moved))
    def _():
        wo_out[...] = wo_l[0, 0].astype(jnp.float32)

    for cp in sent:
        cp.wait_send()


def reduce_grads(wo, w, small, inp, cid):
    nz, nx, ny = grid_of()
    ns, ne = ny * 2, nz * nx
    bf, f32 = jnp.bfloat16, jnp.float32
    rows_o, width = wo.shape[1:]
    rows_w, cb = w.shape[1:]
    rows_n = inp.shape[1]
    n = 3 * nz * nx + 3 * nz + 2 * ns + 8 * ny + 8
    small_block = small.shape[1:]
    return pl.pallas_call(grads_kernel,
        out_shape=(jax.ShapeDtypeStruct((rows_o, width), f32), jax.ShapeDtypeStruct((ns, rows_w, cb), f32),
            jax.ShapeDtypeStruct((ns,) + small_block, f32), jax.ShapeDtypeStruct((rows_n, width), f32)),
        in_specs=[ANY, ANY, ANY, VM], out_specs=(VM, VM, VM, VM),
        scratch_shapes=[pltpu.VMEM((nx - 1, nz, 1, rows_o, width), bf), pltpu.VMEM((nz - 1, 1, rows_o, width), bf),
            pltpu.VMEM((nz, 1, rows_o, width), bf), pltpu.VMEM((rows_o, width), bf),
            pltpu.VMEM((nx - 1, nz, ns, rows_w, cb), bf), pltpu.VMEM((nz - 1, ns, rows_w, cb), bf),
            pltpu.VMEM((nz, ns, rows_w, cb), bf), pltpu.VMEM((ns, rows_w, cb), bf),
            pltpu.VMEM((nx - 1, nz, ns) + small_block, f32), pltpu.VMEM((nz - 1, ns) + small_block, f32),
            pltpu.VMEM((nz, ns) + small_block, f32)]
            + pack_scratch(ny, rows_n, width, bf)
            + [pltpu.SemaphoreType.DMA((3 * nz,)), pltpu.SemaphoreType.DMA((n,)), pltpu.SemaphoreType.DMA((n,))],
        compiler_params=pltpu.CompilerParams(collective_id=cid, has_side_effects=True, vmem_limit_bytes=56 << 20),
        name="reduce_grads")(wo, w, small, inp)


QUERY_HEADS = 32
KEY_VALUE_HEADS = 4
HEAD = 128
EPSILON = 1e-06
THETA = 1000000.0


def normed(raw, gain):
    scale = lax.rsqrt(jnp.mean(raw * raw, axis=-1, keepdims=True) + EPSILON)
    hat = raw * scale
    return scale, hat, hat * gain


def turned(v, cosine, sine):
    return v * cosine + pltpu.roll(v, HEAD // 2, 1) * sine


def turned_back(g, cosine, sine):
    return g * cosine + pltpu.roll(g * sine, HEAD // 2, 1)


def weights_of(queries, keys, mask):
    scores = lax.dot_general(queries, keys, (((1,), (1,)), ((), ())), preferred_element_type=jnp.float32)
    scores = scores * HEAD ** (-0.5) + mask
    highest = jnp.max(scores, axis=-1, keepdims=True)
    powers = jnp.exp(scores - highest)
    return powers * (1.0 / jnp.sum(powers, axis=-1, keepdims=True))


def attend_kernel(q_ref, k_ref, v_ref, gq_ref, gk_ref, cos_ref, sin_ref, mask_ref, o_ref):
    bf = jnp.bfloat16
    cosine, sine = cos_ref[...], sin_ref[...]
    queries = turned(normed(q_ref[...], gq_ref[...])[2], cosine, sine).astype(bf)
    keys = turned(normed(k_ref[...], gk_ref[...])[2], cosine, sine).astype(bf)
    probs = weights_of(queries, keys, mask_ref[...]).astype(bf)
    o_ref[...] = jnp.dot(probs, v_ref[...].astype(bf), preferred_element_type=jnp.float32).astype(bf)


def attend_back_kernel(per, q_ref, k_ref, v_ref, gq_ref, gk_ref, cos_ref, sin_ref, mask_ref, o_ref, do_ref, inv_ref,
                       dq_ref, dk_ref, dv_ref, dgq_ref, dgk_ref, dk_acc, dv_acc):
    bf, f32 = jnp.bfloat16, jnp.float32
    h = pl.program_id(0)
    cosine, sine = cos_ref[...], sin_ref[...]
    gain_q, gain_k = gq_ref[...], gk_ref[...]
    q_scale, q_hat, q_gained = normed(q_ref[...], gain_q)
    k_scale, k_hat, k_gained = normed(k_ref[...], gain_k)
    queries = turned(q_gained, cosine, sine).astype(bf)
    keys = turned(k_gained, cosine, sine).astype(bf)
    probs = weights_of(queries, keys, mask_ref[...])
    out_grad = do_ref[...]
    delta = jnp.sum(out_grad.astype(f32) * o_ref[...].astype(f32), axis=-1, keepdims=True)
    prob_grad = lax.dot_general(out_grad, v_ref[...].astype(bf), (((1,), (1,)), ((), ())), preferred_element_type=f32)
    score_grad = (probs * (prob_grad - delta)).astype(bf)
    factor = HEAD ** (-0.5)
    over_rows = (((0,), (0,)), ((), ()))
    dk_here = lax.dot_general(score_grad, queries, over_rows, preferred_element_type=f32)
    dv_here = lax.dot_general(probs.astype(bf), out_grad, over_rows, preferred_element_type=f32)

    @pl.when(h % per == 0)
    def _():
        dk_acc[...] = dk_here
        dv_acc[...] = dv_here

    @pl.when(h % per != 0)
    def _():
        dk_acc[...] += dk_here
        dv_acc[...] += dv_here

    @pl.when(h == 0)
    def _():
        dgq_ref[...] = jnp.zeros_like(dgq_ref)
        dgk_ref[...] = jnp.zeros_like(dgk_ref)

    def raw_grad(grad, scale, hat, gain, gain_grad_ref):
        gained = turned_back(grad, cosine, sine)
        gain_grad_ref[0:1, :] += jnp.sum(gained * hat, axis=0, keepdims=True)
        inner = gained * gain
        return scale * (inner - hat * jnp.mean(inner * hat, axis=-1, keepdims=True))

    query_grad = jnp.dot(score_grad, keys, preferred_element_type=f32) * factor
    dq_ref[...] = (raw_grad(query_grad, q_scale, q_hat, gain_q, dgq_ref) * inv_ref[...]).astype(bf)

    @pl.when(h % per == per - 1)
    def _():
        dk_ref[...] = (raw_grad(dk_acc[...] * factor, k_scale, k_hat, gain_k, dgk_ref) * inv_ref[...]).astype(bf)
        dv_ref[...] = (dv_acc[...] * inv_ref[...]).astype(bf)


def head_specs(length, heads, kv_heads, per):
    block = (length, HEAD)
    same = lambda h: (0, 0)
    return block, [pl.BlockSpec(block, lambda h: (0, h)), pl.BlockSpec(block, lambda h: (0, heads + h // per)),
        pl.BlockSpec(block, lambda h: (0, heads + kv_heads + h // per)), pl.BlockSpec((1, HEAD), same),
        pl.BlockSpec((1, HEAD), same), pl.BlockSpec(block, same), pl.BlockSpec(block, same),
        pl.BlockSpec((length, length), same)]


def attend(projected, shared, heads, kv_heads):
    length = projected.shape[0]
    block, specs = head_specs(length, heads, kv_heads, heads // kv_heads)
    return pl.pallas_call(attend_kernel, grid=(heads,),
        out_shape=jax.ShapeDtypeStruct((length, heads * HEAD), jnp.bfloat16),
        in_specs=specs, out_specs=pl.BlockSpec(block, lambda h: (0, h)),
        compiler_params=pltpu.CompilerParams(vmem_limit_bytes=56 << 20),
        name="attend")(projected, projected, projected, *shared)


def attend_back(projected, shared, attn, attn_grad, inverse, heads, kv_heads):
    length = projected.shape[0]
    per = heads // kv_heads
    block, specs = head_specs(length, heads, kv_heads, per)
    at_head = pl.BlockSpec(block, lambda h: (0, h))
    at_group = pl.BlockSpec(block, lambda h: (0, h // per))
    small = pl.BlockSpec((8, HEAD), lambda h: (0, 0))
    sds, bf, f32 = jax.ShapeDtypeStruct, jnp.bfloat16, jnp.float32
    return pl.pallas_call(functools.partial(attend_back_kernel, per), grid=(heads,),
        out_shape=(sds((length, heads * HEAD), bf), sds((length, kv_heads * HEAD), bf), sds((length, kv_heads * HEAD), bf),
            sds((8, HEAD), f32), sds((8, HEAD), f32)),
        in_specs=specs + [at_head, at_head, pl.BlockSpec((length, 1), lambda h: (0, 0))],
        out_specs=(at_head, at_group, at_group, small, small),
        scratch_shapes=[pltpu.VMEM(block, f32), pltpu.VMEM(block, f32)],
        compiler_params=pltpu.CompilerParams(vmem_limit_bytes=58 << 20),
        name="attend_back")(projected, projected, projected, *shared, attn, attn_grad, inverse)


def segment_starts(segment):
    index = jnp.arange(segment.shape[0], dtype=jnp.int32)
    same = segment[:, None] == segment[None, :]
    return jnp.min(jnp.where(same, index[None, :], segment.shape[0]), axis=1)


def shards(tokens_in, out_grad, segment_ids, expert_ids, route_weights, attn_gain, qkv_weight, q_gain, k_gain,
           out_weight, moe_gain, expert_in, expert_out):
    f32, bf = jnp.float32, jnp.bfloat16
    n_expert, n_shard = lax.axis_size("expert"), lax.axis_size("shard")
    nd = n_expert * n_shard
    rows, width = tokens_in.shape
    me = lax.axis_index("expert") * n_shard + lax.axis_index("shard")
    heads = QUERY_HEADS // n_shard
    kv_heads = max(1, KEY_VALUE_HEADS // n_shard)
    copies = max(1, n_shard // KEY_VALUE_HEADS)
    q_cols, kv_cols = heads * HEAD, kv_heads * HEAD
    q_all, kv_all = QUERY_HEADS * HEAD, KEY_VALUE_HEADS * HEAD
    wide = qkv_weight.shape[0]

    scaled = (qkv_weight.astype(f32) * attn_gain.astype(f32)[:, None]).astype(bf)

    def by_shard(part, cols, count):
        part = part.reshape(wide, n_shard // count, 1, cols)
        return jnp.broadcast_to(part, (wide, n_shard // count, count, cols)).reshape(wide, n_shard, cols)

    pieces = jnp.concatenate([by_shard(scaled[:, :q_all], q_cols, 1),
        by_shard(scaled[:, q_all:q_all + kv_all], kv_cols, copies),
        by_shard(scaled[:, q_all + kv_all:], kv_cols, copies)], axis=2).transpose(1, 0, 2)
    weights, out_rows, pack = gather_weights(pieces, out_weight, tokens_in, 0)
    weights = weights.reshape(width, -1)
    out_rows = out_rows.reshape(heads * HEAD, width)
    pack = pack.reshape(n_shard * rows, width)
    length = pack.shape[0]

    high = route_weights.astype(bf)
    rest = route_weights - high.astype(f32)
    middle = rest.astype(bf)
    low = (rest - middle.astype(f32)).astype(bf)
    top = expert_ids.shape[1]
    gains = jnp.zeros((rows,), bf)
    at = 0
    for g in (moe_gain, q_gain, k_gain):
        gains = lax.dynamic_update_slice(gains, g, (at,))
        at += g.shape[0]
    extra = jnp.concatenate([expert_ids.astype(bf), high, middle, low, gains[:, None]], axis=1)
    extra = jnp.pad(extra, ((0, 0), (0, 128 - extra.shape[1])))
    both = ("expert", "shard")
    info = lax.all_gather(extra, both, axis=0, tiled=False).astype(f32)
    grads_all = lax.all_gather(out_grad, both, axis=0, tiled=True).reshape(nd, rows, width)
    ids_all = info[:, :, :top]
    weights_all = info[:, :, top:2 * top] + info[:, :, 2 * top:3 * top] + info[:, :, 3 * top:4 * top]
    gain_col = info[:, :, 4 * top]
    g0, g1, g2 = moe_gain.shape[0], q_gain.shape[0], k_gain.shape[0]
    moe_scale = gain_col[:, :g0].reshape(-1)
    query_gain = gain_col[:, g0:g0 + g1].reshape(-1)
    key_gain = gain_col[:, g0 + g1:g0 + g1 + g2].reshape(-1)

    pack_f32 = pack.astype(f32)
    inverse = lax.rsqrt(jnp.mean(pack_f32 * pack_f32, axis=-1, keepdims=True) + EPSILON)
    projected = jnp.dot(pack, weights, preferred_element_type=f32) * inverse
    segment = segment_ids[0]
    index = jnp.arange(length, dtype=jnp.int32)
    position = (index - segment_starts(segment)).astype(f32)
    freqs = jnp.exp(jnp.arange(HEAD // 2, dtype=f32) * (-2.0 * math.log(THETA) / HEAD))
    angles = position[:, None] * freqs[None, :]
    cosine, sine = jnp.cos(angles), jnp.sin(angles)
    allowed = (segment[:, None] == segment[None, :]) & (index[None, :] <= index[:, None])
    shared = (query_gain[None], key_gain[None], jnp.concatenate([cosine, cosine], axis=1),
        jnp.concatenate([-sine, sine], axis=1), jnp.where(allowed, 0.0, -1e30).astype(f32))
    attn_flat = attend(projected, shared, heads, kv_heads)
    mixed = jnp.dot(attn_flat, out_rows, preferred_element_type=f32).astype(bf)
    hidden_state = tokens_in.astype(f32) + pack_reduce(mixed.reshape(n_shard, rows, width), 2)
    hidden_inverse = lax.rsqrt(jnp.mean(hidden_state * hidden_state, axis=-1, keepdims=True) + EPSILON)
    hidden_norm = hidden_state * hidden_inverse
    moe_in = (hidden_norm * moe_scale).astype(bf)

    cap = max(2, 2 * rows * top // nd)
    hit = ids_all == me.astype(f32)
    any_hit = jnp.any(hit, axis=-1)
    gate = jnp.sum(jnp.where(hit, weights_all, 0.0), axis=-1)
    lower = (jnp.arange(rows)[:, None] <= jnp.arange(rows)[None, :]).astype(bf)
    rank = jnp.dot(any_hit.astype(bf), lower, preferred_element_type=f32) - 1.0
    chosen = (jnp.arange(cap, dtype=f32)[None, :, None] == rank[:, None, :]) & any_hit[:, None, :]
    slot_gate = jnp.sum(jnp.where(chosen, gate[:, None, :], 0.0), axis=-1)
    select = chosen.astype(bf)
    experts = (moe_in, select, slot_gate, grads_all, expert_in[0], expert_out[0])
    if 16 * nd * rows * width // 5 <= 28 << 20:
        in_rows, grad_rows, hidden, pre_grad, out_terms, moe_grad = expert_reduce(*experts, 3)
    else:
        in_rows, grad_rows, hidden, pre_grad, out_terms, rows_grad = expert_pass(*experts, 1)
        moe_grad = reduce_rows(rows_grad.reshape(nd, cap, width), select, 5)
    expert_in_grad = jnp.einsum("rd,rc->dc", in_rows, pre_grad, preferred_element_type=f32)[None]
    expert_out_grad = jnp.einsum("rf,rd->fd", hidden, grad_rows, preferred_element_type=f32)[None]

    scaled_grad = moe_grad * moe_scale
    moe_gain_grad = jnp.sum(moe_grad * hidden_norm, axis=0)
    residual = out_grad.astype(f32) + hidden_inverse * (
        scaled_grad - hidden_norm * jnp.mean(scaled_grad * hidden_norm, axis=-1, keepdims=True))
    residual_pack = pack_gather(residual.astype(bf), 6).reshape(length, width)
    moe_sum = lax.psum_scatter(out_terms.reshape(nd * rows, width), both, scatter_dimension=0, tiled=True).astype(f32)
    block_output = (hidden_state + moe_sum).astype(bf)
    out_term = jnp.einsum("tc,td->cd", attn_flat, residual_pack, preferred_element_type=f32).astype(bf)
    attn_grad = jnp.einsum("td,cd->tc", residual_pack, out_rows, preferred_element_type=f32).astype(bf)
    query_part, key_part, value_part, query_gain_grad, key_gain_grad = attend_back(projected, shared, attn_flat, attn_grad,
        inverse, heads, kv_heads)
    query_gain_grad, key_gain_grad = query_gain_grad[0], key_gain_grad[0]
    projected_grad = jnp.concatenate([query_part, key_part, value_part], axis=1)
    qkv_term = jnp.einsum("td,tc->dc", pack, projected_grad, preferred_element_type=f32).astype(bf)
    input_term = jnp.einsum("tc,dc->td", projected_grad, weights, preferred_element_type=f32).astype(bf)

    def lanes(v):
        v = v.reshape(nd, -1)
        return jnp.pad(v, ((0, 0), (0, 128 - v.shape[1])))[:, None]

    expert_in_grad, expert_out_grad, input_term = lax.optimization_barrier((expert_in_grad, expert_out_grad, input_term))
    small = jnp.concatenate([lanes(moe_gain_grad), lanes(query_gain_grad), lanes(key_gain_grad),
        jnp.zeros((nd, 5, 128), f32)], axis=1)
    out_weight_grad, qkv_part, small_sum, input_sum = reduce_grads(out_term.reshape(n_expert, -1, width),
        qkv_term.reshape(nd, wide, -1), small, input_term.reshape(n_shard, rows, width), 7)
    small_sum = jnp.sum(small_sum, axis=0)

    def whole_cols(part, count):
        part = part.transpose(1, 0, 2).reshape(wide, n_shard // count, count, -1)
        return jnp.sum(part, axis=2).reshape(wide, -1)

    raw = jnp.concatenate([whole_cols(qkv_part[:, :, :q_cols], 1), whole_cols(qkv_part[:, :, q_cols:q_cols + kv_cols], copies),
        whole_cols(qkv_part[:, :, q_cols + kv_cols:], copies)], axis=1)
    attn_gain_grad = jnp.sum(raw * qkv_weight.astype(f32), axis=1)
    qkv_weight_grad = raw * attn_gain.astype(f32)[:, None]
    own = tokens_in.astype(f32)
    own_norm = own * lax.rsqrt(jnp.mean(own * own, axis=-1, keepdims=True) + EPSILON)
    input_grad = (residual + input_sum - own_norm * jnp.mean(input_sum * own_norm, axis=-1, keepdims=True)).astype(bf)
    return (block_output, input_grad, attn_gain_grad, qkv_weight_grad, small_sum[1, :g1], small_sum[2, :g2],
        out_weight_grad, small_sum[0, :g0], expert_in_grad, expert_out_grad)


def solution(mesh):
    both = ("expert", "shard")
    row, rows2, rows3 = P(both), P(both, None), P(both, None, None)
    return jax.shard_map(
        shards, mesh=mesh,
        in_specs=(rows2, rows2, P("expert", None), rows2, rows2, row, rows2, row, row, rows2, row, rows3, rows3),
        out_specs=(rows2, rows2, row, rows2, row, row, rows2, row, rows3, rows3),
        check_vma=False,
    )
```
